8 devices in a mesh: b: 4 (over z, y, x), a: 2 (over core).
Axes of the slice: x: 2, y: 2, z: 1, core: 2. Of those that a mesh axis runs over, the one named last changes fastest.
Arguments:
- u: float32 [256, 256, 256], P(None, 'a', 'b')
- g: float32 [130, 256, 256], P('a', 'b')
Outputs:
- output: float32 [256, 256, 256], P(None, 'a', 'b')
All inputs are finite; a program needn't handle non-finite values.
Results may differ from the reference program's by a relative error of at most 0.001.
Values are sent between devices in bfloat16 or wider.
A program may use at most 1 GiB of HBM per device.

```python
import math
import jax
import jax.numpy as jnp
from jax import lax

N = 256
KX = 130

HI = lax.Precision.HIGHEST


def _trig(rows, cols):
    r = jnp.arange(rows, dtype=jnp.int32)[:, None]
    c = jnp.arange(cols, dtype=jnp.int32)[None, :]
    ang = ((r * c) % N).astype(jnp.float32) * (2.0 * math.pi / N)
    return jnp.cos(ang), jnp.sin(ang)


def _ksq():
    kx = jnp.arange(KX, dtype=jnp.int32)
    k = jnp.arange(N, dtype=jnp.int32)
    k = jnp.where(k <= N // 2, k, k - N)
    k2 = kx[:, None, None] ** 2 + k[None, :, None] ** 2 + k[None, None, :] ** 2
    return k2.astype(jnp.float32)


def setup_inputs(seed: int = 0) -> dict:
    k1, k2 = jax.random.split(jax.random.key(seed))
    u = jax.random.normal(k1, (N, N, N), jnp.float32)
    r = jax.random.uniform(k2, (KX, N, N), jnp.float32, -1.0, 1.0)
    g = (1.0 + 0.5 * r) / (1.0 + _ksq() / (N / 4.0) ** 2)
    g = g / jnp.sqrt(jnp.mean(g[: N // 2 + 1] ** 2))
    return {"u": u, "g": g.astype(jnp.float32)}


def _line(xr, xi, c, s, form, sign):
    f = lambda p, q: jnp.einsum(form, p.astype(jnp.float32), q.astype(jnp.float32), precision=HI)
    return f(xr, c) + sign * f(xi, s), f(xi, c) - sign * f(xr, s)


def reference(u, g):
    c, s = _trig(N, N)
    cx, sx = _trig(KX, N)
    k = jnp.arange(KX)
    keep = (k <= N // 2).astype(jnp.float32)
    wgt = jnp.where((k == 0) | (k == N // 2), 1.0, 2.0) * keep / N
    u2 = u.reshape(N, N * N)
    xr = jnp.dot(cx * keep[:, None], u2, precision=HI, preferred_element_type=jnp.float32).reshape(KX, N, N)
    xi = jnp.dot(-sx * keep[:, None], u2, precision=HI, preferred_element_type=jnp.float32).reshape(KX, N, N)
    xr, xi = _line(xr, xi, c, s, "xyz,yk->xkz", 1.0)
    xr, xi = _line(xr, xi, c, s, "xyz,zk->xyk", 1.0)
    xr, xi = xr * g, xi * g
    xr, xi = _line(xr, xi, c / N, s / N, "xyz,zk->xyk", -1.0)
    xr, xi = _line(xr, xi, c / N, s / N, "xyz,yk->xkz", -1.0)
    ar = (cx * wgt[:, None]).T
    ai = (sx * wgt[:, None]).T
    w = jnp.dot(ar, xr.reshape(KX, N * N), precision=HI, preferred_element_type=jnp.float32) - jnp.dot(ai, xi.reshape(KX, N * N), precision=HI, preferred_element_type=jnp.float32)
    return w.reshape(N, N, N)
```

```python
import functools
import math
import jax
import jax.numpy as jnp
import numpy as np
from jax import lax
from jax.experimental import pallas as pl
from jax.experimental.pallas import tpu as pltpu
from jax.sharding import PartitionSpec as P

HI = lax.Precision.HIGHEST
F32 = jnp.float32
KC = 5


def _trig(n, rows, cols):
    r = np.arange(rows)[:, None]
    c = np.arange(cols)[None, :]
    ang = ((r * c) % n).astype(np.float32) * np.float32(2.0 * math.pi / n)
    return np.cos(ang.astype(np.float64)), np.sin(ang.astype(np.float64))


def _xtables(n, kx, pad):
    cx, sx = _trig(n, kx, n)
    k = np.arange(kx)
    keep = (k <= n // 2).astype(np.float64)
    wgt = np.where((k == 0) | (k == n // 2), 1.0, 2.0) * keep / n
    fwd = np.zeros((pad, n))
    fwd[: 2 * kx] = np.stack([cx * keep[:, None], -sx * keep[:, None]], 1).reshape(2 * kx, n)
    inv = np.zeros((pad, n))
    inv[: 2 * kx] = np.stack([cx * wgt[:, None], -sx * wgt[:, None]], 1).reshape(2 * kx, n)
    return fwd.astype(np.float32), inv.T.astype(np.float32).copy()


def _ytables(n, nb):
    c, s = _trig(n, n, n)
    full = np.block([[c, -s], [s, c]])
    w = full.reshape(2 * n, 2, nb, n // nb).transpose(0, 2, 1, 3).reshape(2 * n, 2 * n)
    inv = (full.T / n).reshape(2, nb, n // nb, 2 * n).transpose(1, 0, 2, 3)
    inv = inv.reshape(2 * n, 2, 2, n // 2).transpose(0, 2, 1, 3).reshape(2 * n, 2 * n)
    return w.astype(np.float32), inv.astype(np.float32)


def _dot(p, q):
    return jnp.dot(p, q, precision=HI, preferred_element_type=F32)


def _xfwd(t_ref, u_ref, o_ref):
    x, zb, y = u_ref.shape
    k = o_ref.shape[0]
    src = u_ref.reshape(x * zb, y)
    dst = o_ref.reshape(k * zb, y)
    for z in range(0, zb, 2):
        rhs = jnp.concatenate([src[pl.ds(z + i, x, stride=zb), :] for i in range(2)], axis=1)
        out = _dot(t_ref[...], rhs)
        for i in range(2):
            dst[pl.ds(z + i, k, stride=zb), :] = out[:, i * y:(i + 1) * y]


def _spectral(nb, p_ref, g_ref, wy_ref, cs_ref, wi_ref, q_ref,
              xb, sf, r, v, qs, gv, csv, wiv,
              load_sem, xa_send, xa_recv, xl_sem, f_send, f_recv, b_send, b_recv, q_send, q_recv, ql_sem):
    b, a = lax.axis_index("b"), lax.axis_index("a")
    other = 1 - a
    nkx = g_ref.shape[0]
    nchunk = nkx // KC
    zb, n = r.shape[1] // nb, r.shape[1]
    bx, by = lax.rem(b, 2), lax.div(b, 2)
    peers = [lax.rem(by + d // 2, 2) * 2 + lax.rem(bx + d % 2, 2) for d in (1, 2, 3)]
    MESH = pl.DeviceIdType.MESH

    def ck(i):
        return pl.ds(i * KC, KC)

    def ck2(i):
        return pl.ds(i * 2 * KC, 2 * KC)

    def prow(owner, i):
        return p_ref.at[pl.ds(owner * 2 * nkx + i * 2 * KC, 2 * KC)]

    loads = [pltpu.make_async_copy(s, d, load_sem.at[i]) for i, (s, d) in enumerate(
        [(g_ref, gv), (cs_ref, csv), (wi_ref, wiv)])]

    def xlocal(i):
        return pltpu.make_async_copy(prow(a, i), xb.at[a, ck2(i)], xl_sem.at[i])

    def xremote(i):
        return pltpu.make_async_remote_copy(
            prow(other, i), xb.at[a, ck2(i)], xa_send.at[i], xa_recv.at[i],
            device_id=(b, other), device_id_type=MESH)

    def fwd(i, d):
        return pltpu.make_async_remote_copy(
            sf.at[ck(i), peers[d]], r.at[ck(i), pl.ds(b * zb, zb)], f_send.at[d, i], f_recv.at[d, i],
            device_id=(peers[d], a), device_id_type=MESH)

    def bwd(i, d):
        return pltpu.make_async_remote_copy(
            r.at[ck(i), pl.ds(peers[d] * zb, zb)], v.at[ck(i), b], b_send.at[d, i], b_recv.at[d, i],
            device_id=(peers[d], a), device_id_type=MESH)

    def qlocal(i):
        return pltpu.make_async_copy(qs.at[a, ck(i)], q_ref.at[a, ck(i)], ql_sem.at[i])

    def qremote(i):
        return pltpu.make_async_remote_copy(
            qs.at[other, ck(i)], q_ref.at[a, ck(i)], q_send.at[i], q_recv.at[i],
            device_id=(b, other), device_id_type=MESH)

    barrier = pltpu.get_barrier_semaphore()
    for dev in [(b, other)] + [(pb, a) for pb in peers]:
        pl.semaphore_signal(barrier, inc=1, device_id=dev, device_id_type=MESH)

    @pl.loop(0, nchunk)
    def _(i):
        xlocal(i).start()

    pl.semaphore_wait(barrier, 4)

    @pl.loop(0, nchunk)
    def _(i):
        xremote(i).start()

    for c in loads:
        c.start()

    @pl.loop(0, nchunk)
    def _(i):
        xlocal(i).wait()
        xremote(i).wait_recv()
        x = jnp.concatenate(
            [jnp.concatenate([xb[h, (i * KC + j) * 2 + c] for j in range(KC)]) for c in range(2) for h in range(2)], axis=1)
        out = _dot(x, wy_ref[...])
        for k in range(nb):
            sf[ck(i), k] = out[:, k * 128:(k + 1) * 128].reshape(KC, zb, 128)
        r[ck(i), pl.ds(b * zb, zb)] = sf[ck(i), b]
        for d in range(3):
            fwd(i, d).start()

    for c in loads:
        c.wait()
    lane = lax.broadcasted_iota(jnp.int32, (n, 128), 1)
    sign = jnp.where(lane < 64, 1.0, -1.0).astype(F32)

    @pl.loop(0, nchunk)
    def _(i):
        for d in range(3):
            fwd(i, d).wait_recv()

        def cat(parts):
            return jnp.concatenate(parts, axis=1)

        e = _dot(csv[...], cat([r[i * KC + j] for j in range(KC)]))
        parts = []
        for j in range(KC):
            cols = slice(j * 128, (j + 1) * 128)
            g1 = gv[i * KC + j] * (1.0 / n)
            gt = jnp.transpose(jnp.concatenate([g1, g1], axis=0))
            parts.append((e[:n, cols] + sign * pltpu.roll(e[n:, cols], 64, 1)) * gt)
        e = _dot(csv[...], cat(parts))
        for j in range(KC):
            cols = slice(j * 128, (j + 1) * 128)
            r[i * KC + j] = e[:n, cols] - sign * pltpu.roll(e[n:, cols], 64, 1)
        v[ck(i), b] = r[ck(i), pl.ds(b * zb, zb)]
        for d in range(3):
            bwd(i, d).start()

    @pl.loop(0, nchunk)
    def _(i):
        for d in range(3):
            bwd(i, d).wait_recv()
        x = jnp.concatenate([v[ck(i), k].reshape(KC * zb, 128) for k in range(nb)], axis=1)
        out = _dot(x, wiv[...])
        for h in range(2):
            for c in range(2):
                m = h * 2 + c
                qs[h, ck(i), c] = out[:, m * 128:(m + 1) * 128].reshape(KC, zb, 128)
        qremote(i).start()
        qlocal(i).start()

    @pl.loop(0, nchunk)
    def _(i):
        xremote(i).wait_send()
        for d in range(3):
            fwd(i, d).wait_send()
            bwd(i, d).wait_send()
        qlocal(i).wait()
        qremote(i).wait()


def _xinv(t_ref, q_ref, o_ref):
    k, zb, y = q_ref.shape
    x = o_ref.shape[0]
    src = q_ref.reshape(k * zb, y)
    dst = o_ref.reshape(x * zb, y)
    for z in range(0, zb, 2):
        rhs = jnp.concatenate([src[pl.ds(z + i, k, stride=zb), :] for i in range(2)], axis=1)
        out = _dot(t_ref[...], rhs)
        for i in range(2):
            dst[pl.ds(z + i, x, stride=zb), :] = out[:, i * y:(i + 1) * y]


def solution(mesh):
    na, nb = mesh.shape["a"], mesh.shape["b"]

    def local(u, g):
        n, ya, zb = u.shape
        nkx = g.shape[0]
        kx = nkx * na
        rows = 2 * kx
        pad = -(-rows // 8) * 8
        tf, ti = _xtables(n, kx, pad)
        wy, wi = _ytables(n, nb)
        c, s = _trig(n, n, n)
        cs = np.concatenate([c, s]).astype(np.float32)
        zt = 8
        ut = jnp.transpose(u, (0, 2, 1))
        vm = pltpu.CompilerParams(vmem_limit_bytes=60 << 20)
        p = pl.pallas_call(
            _xfwd, grid=(zb // zt,), name="xfwd",
            in_specs=[pl.BlockSpec((pad, n), lambda i: (0, 0)), pl.BlockSpec((n, zt, ya), lambda i: (0, i, 0))],
            out_specs=pl.BlockSpec((pad, zt, ya), lambda i: (0, i, 0)),
            out_shape=jax.ShapeDtypeStruct((pad, zb, ya), F32), compiler_params=vm,
        )(tf, ut)
        nchunk = nkx // KC
        anyspec = pl.BlockSpec(memory_space=pl.ANY)
        dma = pltpu.SemaphoreType.DMA
        q = pl.pallas_call(
            functools.partial(_spectral, nb), name="spectral",
            in_specs=[anyspec, anyspec, pl.BlockSpec(memory_space=pltpu.VMEM), anyspec, anyspec],
            out_specs=anyspec,
            out_shape=jax.ShapeDtypeStruct((na, nkx, 2, zb, ya), F32),
            scratch_shapes=[
                pltpu.VMEM((na, nkx * 2, zb, ya), F32),
                pltpu.VMEM((nkx, nb, zb, 128), F32),
                pltpu.VMEM((nkx, n, 128), F32),
                pltpu.VMEM((nkx, nb, zb, 128), F32),
                pltpu.VMEM((na, nkx, 2, zb, ya), F32),
                pltpu.VMEM(g.shape, F32), pltpu.VMEM(cs.shape, F32), pltpu.VMEM(wi.shape, F32),
                dma((3,)), dma((nchunk,)), dma((nchunk,)), dma((nchunk,)),
                dma((3, nchunk)), dma((3, nchunk)), dma((3, nchunk)), dma((3, nchunk)),
                dma((nchunk,)), dma((nchunk,)), dma((nchunk,)),
            ],
            compiler_params=pltpu.CompilerParams(
                collective_id=0, has_side_effects=True, vmem_limit_bytes=67043328),
        )(p, g, wy, cs, wi)
        w = pl.pallas_call(
            _xinv, grid=(zb // zt,), name="xinv",
            in_specs=[pl.BlockSpec((n, rows), lambda i: (0, 0)), pl.BlockSpec((rows, zt, ya), lambda i: (0, i, 0))],
            out_specs=pl.BlockSpec((n, zt, ya), lambda i: (0, i, 0)),
            out_shape=jax.ShapeDtypeStruct((n, zb, ya), F32), compiler_params=vm,
        )(ti[:, :rows], q.reshape(rows, zb, ya))
        return jnp.transpose(w, (0, 2, 1))

    return jax.shard_map(local, mesh=mesh, in_specs=(P(None, "a", "b"), P("a", "b", None)), out_specs=P(None, "a", "b"), check_vma=False)
```

```python
import functools
import math
import jax
import jax.numpy as jnp
import numpy as np
from jax import lax
from jax.experimental import pallas as pl
from jax.experimental.pallas import tpu as pltpu
from jax.sharding import PartitionSpec as P

HI = lax.Precision.HIGHEST
F32, BF16 = jnp.float32, jnp.bfloat16
MESH = pl.DeviceIdType.MESH
KC = 5
KA = 13
NLAST = 2
ZT = 8
ROWS = 136
HALF = ROWS // 2
TROWS = 144


def _trig(n, rows, cols):
    r = np.arange(rows)[:, None]
    c = np.arange(cols)[None, :]
    ang = ((r * c) % n).astype(np.float32) * np.float32(2.0 * math.pi / n)
    return np.cos(ang.astype(np.float64)), np.sin(ang.astype(np.float64))


def _xforward(n, kx, na):
    cx, sx = _trig(n, kx, n)
    keep = (np.arange(kx) <= n // 2).astype(np.float64)[:, None]
    t = np.zeros((na, 2, HALF, n))
    t[:, 0, : kx // na] = (cx * keep).reshape(na, kx // na, n)
    t[:, 1, : kx // na] = (-sx * keep).reshape(na, kx // na, n)
    t = np.pad(t.reshape(na, ROWS, n), ((0, 0), (0, TROWS - ROWS), (0, 0)))
    return np.concatenate([t, t[:1]]).reshape((na + 1) * TROWS, n).astype(np.float32)


def _xinverse(n, kx, na):
    cx, sx = _trig(n, kx, n)
    k = np.arange(kx)
    wgt = (np.where((k == 0) | (k == n // 2), 1.0, 2.0) * (k <= n // 2) / n)[:, None]
    t = np.stack([cx * wgt, -sx * wgt], 1).reshape(na, kx // na // KC, KC, 2, n)
    return t.transpose(1, 0, 2, 3, 4).reshape(2 * kx, n).T.astype(np.float32).copy()


def _ytables(n, nb):
    c, s = _trig(n, n, n)
    full = np.block([[c, -s], [s, c]])
    w = full.reshape(2 * n, 2, nb, n // nb).transpose(0, 2, 1, 3).reshape(2 * n, 2 * n)
    inv = (full.T / n).reshape(2, nb, n // nb, 2 * n).transpose(1, 0, 2, 3)
    inv = inv.reshape(2 * n, 2, 2, n // 2).transpose(0, 2, 1, 3).reshape(2 * n, 2 * n)
    return w.astype(np.float32), inv.astype(np.float32)


def _split(x):
    hi = x.astype(BF16)
    x = x - hi.astype(F32)
    mid = x.astype(BF16)
    return hi, mid, (x - mid.astype(F32)).astype(BF16)


def _nsplit(x):
    hi = x.astype(jnp.bfloat16)
    x = x - hi.astype(np.float32)
    mid = x.astype(jnp.bfloat16)
    return hi, mid, (x - mid.astype(np.float32)).astype(jnp.bfloat16)


def _mm(p, q):
    d = functools.partial(jnp.dot, preferred_element_type=F32)
    return d(p[0], q[2]) + d(p[1], q[1]) + d(p[2], q[0]) + d(p[0], q[1]) + d(p[1], q[0]) + d(p[0], q[0])


def _dot(p, q):
    return jnp.dot(p, q, precision=HI, preferred_element_type=F32)


def _cat(parts):
    return jnp.concatenate(parts, axis=1)


def _spectral(nb, u_ref, g_ref, t_ref, wy_ref, cs_ref, wi_ref, ai_ref, acc_ref, ql_ref,
              uv, xb, ps, sf, r, v, qx, ws, gv, tv, wv, csv, aiv, tsp, wysp, wisp,
              load_sem, u_sem, g_sem, xa_send, xa_recv, fa_send, fa_recv, f_send, f_recv,
              b_send, b_recv, q_send, q_recv, ql_sem, w_sem):
    b, a = lax.axis_index("b"), lax.axis_index("a")
    other = 1 - a
    nkx = g_ref.shape[0]
    nchunk, npiece = nkx // KC, nkx // KA
    nbulk = nchunk - NLAST
    n = r.shape[1]
    zb = n // nb
    nz = zb // ZT
    y = 128
    bx, by = lax.rem(b, 2), lax.div(b, 2)
    peers = [lax.rem(by + d // 2, 2) * 2 + lax.rem(bx + d % 2, 2) for d in (1, 2, 3)]
    us = uv.shape[0]

    def ck(i):
        return pl.ds(i * KC, KC)

    def ka(i):
        return pl.ds(i * KA, KA)

    loads = [pltpu.make_async_copy(s, d, load_sem.at[i]) for i, (s, d) in enumerate(
        [(t_ref, tv), (wy_ref, wv), (wi_ref, wv), (cs_ref, csv), (ai_ref, aiv)])]
    gs = gv.shape[0]

    def gload(i):
        return pltpu.make_async_copy(g_ref.at[ck(i)], gv.at[lax.rem(i, gs)], g_sem.at[lax.rem(i, gs)])

    def uload(z):
        return pltpu.make_async_copy(
            u_ref.at[:, pl.ds(z * ZT, ZT)], uv.at[lax.rem(z, us)], u_sem.at[lax.rem(z, us)])

    def xremote(z):
        return pltpu.make_async_remote_copy(
            ps.at[z], xb.at[z, a], xa_send.at[z], xa_recv.at[z], device_id=(b, other), device_id_type=MESH)

    def fwda(i, d):
        return pltpu.make_async_remote_copy(
            sf.at[ka(i), peers[d], pl.ds(0, ZT)], r.at[ka(i), pl.ds(b * zb, ZT)],
            fa_send.at[d, i], fa_recv.at[d, i], device_id=(peers[d], a), device_id_type=MESH)

    def fwd(i, d):
        return pltpu.make_async_remote_copy(
            sf.at[ck(i), peers[d], pl.ds(ZT, zb - ZT)], r.at[ck(i), pl.ds(b * zb + ZT, zb - ZT)],
            f_send.at[d, i], f_recv.at[d, i], device_id=(peers[d], a), device_id_type=MESH)

    def bwd(i, d):
        return pltpu.make_async_remote_copy(
            r.at[ck(i), pl.ds(peers[d] * zb, zb)], v.at[ck(i), b], b_send.at[d, i], b_recv.at[d, i],
            device_id=(peers[d], a), device_id_type=MESH)

    def qsrc(i):
        return ps.at[:, pl.ds(i * 2 * KC, 2 * KC)]

    def qremote(i):
        return pltpu.make_async_remote_copy(
            qsrc(i), qx.at[:, i, a], q_send.at[i], q_recv.at[i], device_id=(b, other), device_id_type=MESH)

    def qlast(i):
        return pltpu.make_async_remote_copy(
            qsrc(i), ql_ref.at[:, i - nbulk, a], q_send.at[i], q_recv.at[i],
            device_id=(b, other), device_id_type=MESH)

    def qlocal(i):
        return pltpu.make_async_copy(qx.at[:, i, a], ql_ref.at[:, i - nbulk, a], ql_sem.at[i - nbulk])

    def wstore(z):
        return pltpu.make_async_copy(
            ws.at[lax.rem(z, 2)], acc_ref.at[pl.ds(z * ZT, ZT)], w_sem.at[lax.rem(z, 2)])

    barrier = pltpu.get_barrier_semaphore()
    for dev in [(b, other)] + [(pb, a) for pb in peers]:
        pl.semaphore_signal(barrier, inc=1, device_id=dev, device_id_type=MESH)
    loads[0].start()
    for z in range(us):
        uload(z).start()
    for c in (loads[1], loads[3], loads[4]):
        c.start()
    for i in range(gs):
        gload(i).start()

    src = uv.reshape(us * n * ZT, y)
    own = xb.reshape(nz * 2 * ROWS * ZT, y)
    sent = ps.reshape(nz * ROWS * ZT, y)

    def split_table(dst, step):
        @pl.loop(0, wv.shape[0] // step)
        def _(i):
            rows = pl.ds(i * step, step)
            for m, part in enumerate(_split(wv[rows, :])):
                dst[m, rows, :] = part

    def xhalf(zi, z, rhs, first, dst, base):
        rows = pl.ds(pl.multiple_of(first * TROWS, 16), TROWS)
        out = _mm([tsp[m, rows, :] for m in range(3)], rhs)
        for i in range(2):
            dst[pl.ds(base * ROWS * ZT + z + i, ROWS, stride=ZT), :] = out[:ROWS, i * y:(i + 1) * y]

    def xblock(zi, halves):
        slot = lax.rem(zi, us)
        for z in range(0, ZT, 2):
            rhs = _split(_cat([src[pl.ds(slot * n * ZT + z + i, n, stride=ZT), :] for i in range(2)]))
            if 1 in halves:
                xhalf(zi, z, rhs, a + 1, sent, zi)
            if 0 in halves:
                xhalf(zi, z, rhs, a, own, zi * 2 + a)

    loads[0].wait()
    for m, part in enumerate(_split(tv[...])):
        tsp[m] = part
    uload(0).wait()
    xblock(0, (1,))
    pl.semaphore_wait(barrier, 4)
    xremote(0).start()
    xblock(0, (0,))
    loads[1].wait()
    split_table(wysp, 128)
    loads[2].start()
    xremote(0).wait_recv()

    @pl.loop(0, npiece)
    def _(i):
        x = _split(_cat([xb[0, h, pl.ds(c * HALF + i * KA, KA)].reshape(KA * ZT, y)
                         for c in range(2) for h in range(2)]))
        out = _mm(x, [wysp[m] for m in range(3)])
        for k in range(nb):
            sf[ka(i), k, pl.ds(0, ZT)] = out[:, k * y:(k + 1) * y].reshape(KA, ZT, y)
        r[ka(i), pl.ds(b * zb, ZT)] = sf[ka(i), b, pl.ds(0, ZT)]
        for d in range(3):
            fwda(i, d).start()

    @pl.loop(1, nz)
    def _(z):
        @pl.when(z + us - 1 < nz)
        def _():
            uload(z + us - 1).start()
        uload(z).wait()
        xblock(z, (1, 0))
        xremote(z).start()

    @pl.loop(1, nz)
    def _(z):
        xremote(z).wait_recv()

    zr = zb - ZT

    @pl.loop(0, nchunk)
    def _(i):
        x = _cat([jnp.concatenate([xb[pl.ds(1, nz - 1), h, c * HALF + i * KC + j].reshape(zr, y) for j in range(KC)])
                  for c in range(2) for h in range(2)])
        out = _mm(_split(x), [wysp[m] for m in range(3)])
        for k in range(nb):
            sf[ck(i), k, pl.ds(ZT, zr)] = out[:, k * y:(k + 1) * y].reshape(KC, zr, y)
        r[ck(i), pl.ds(b * zb + ZT, zr)] = sf[ck(i), b, pl.ds(ZT, zr)]
        for d in range(3):
            fwd(i, d).start()

    for c in loads[2:]:
        c.wait()
    split_table(wisp, 128)
    lane = lax.broadcasted_iota(jnp.int32, (n, y), 1)
    sign = jnp.where(lane < y // 2, 1.0, -1.0).astype(F32)

    @pl.loop(0, npiece)
    def _(i):
        for d in range(3):
            fwda(i, d).wait_recv()

    @pl.loop(0, nchunk)
    def _(i):
        for d in range(3):
            fwd(i, d).wait_recv()
        gload(i).wait()
        e = _dot(csv[...], _cat([r[i * KC + j] for j in range(KC)]))
        parts = []
        for j in range(KC):
            cols = slice(j * y, (j + 1) * y)
            g1 = gv[lax.rem(i, gs), j] * (1.0 / n)
            gt = jnp.transpose(jnp.concatenate([g1, g1], axis=0))
            parts.append((e[:n, cols] + sign * pltpu.roll(e[n:, cols], y // 2, 1)) * gt)

        @pl.when(i + gs < nchunk)
        def _():
            gload(i + gs).start()
        e = _dot(csv[...], _cat(parts))
        for j in range(KC):
            cols = slice(j * y, (j + 1) * y)
            r[i * KC + j] = e[:n, cols] - sign * pltpu.roll(e[n:, cols], y // 2, 1)
        v[ck(i), b] = r[ck(i), pl.ds(b * zb, zb)]
        for d in range(3):
            bwd(i, d).start()

    @pl.loop(0, nz)
    def _(z):
        xremote(z).wait_send()

    def yinverse(i):
        for d in range(3):
            bwd(i, d).wait_recv()
        out = _mm(_split(_cat([v[ck(i), k].reshape(KC * zb, y) for k in range(nb)])), [wisp[m] for m in range(3)])

        def tile(h, c, j):
            m = h * 2 + c
            return out[j * zb:(j + 1) * zb, m * y:(m + 1) * y].reshape(nz, ZT, y)

        for c in range(2):
            for j in range(KC):
                t0, t1 = tile(0, c, j), tile(1, c, j)
                qx[:, i, a, j * 2 + c] = jnp.where(a == 0, t0, t1)
                ps[:, i * 2 * KC + j * 2 + c] = jnp.where(a == 0, t1, t0)

    @pl.loop(0, nbulk)
    def _(i):
        yinverse(i)
        qremote(i).start()

    @pl.loop(0, nbulk)
    def _(i):
        qremote(i).wait_recv()

    qrows = nchunk * 4 * KC
    brows = nbulk * 4 * KC
    qflat = qx.reshape(nz * qrows * ZT, y)

    @pl.loop(0, nz)
    def _(zi):
        @pl.when(zi >= 2)
        def _():
            wstore(zi - 2).wait()
        for z in range(0, ZT, 2):
            rhs = _cat([qflat[pl.ds(zi * qrows * ZT + z + i, brows, stride=ZT), :] for i in range(2)])
            out = _dot(aiv[...], rhs)
            for i in range(2):
                ws[lax.rem(zi, 2), z + i] = out[:, i * y:(i + 1) * y]
        wstore(zi).start()

    @pl.loop(nbulk, nchunk)
    def _(i):
        yinverse(i)
        qlast(i).start()
        qlocal(i).start()

    for z in (nz - 2, nz - 1):
        wstore(z).wait()

    @pl.loop(0, npiece)
    def _(i):
        for d in range(3):
            fwda(i, d).wait_send()

    @pl.loop(0, nchunk)
    def _(i):
        for d in range(3):
            fwd(i, d).wait_send()
            bwd(i, d).wait_send()

    @pl.loop(0, nbulk)
    def _(i):
        qremote(i).wait_send()

    @pl.loop(nbulk, nchunk)
    def _(i):
        qlocal(i).wait()
        qlast(i).wait()


def _finish(t_ref, w_ref, q_ref, o_ref, wv, qv, ov, in_sem, q_sem, out_sem):
    nz, x, zt, y = ov.shape
    k = q_ref.shape[1]
    src = qv.reshape(nz * k * zt, y)
    dst = ov.reshape(nz * x * zt, y)

    def load(i):
        return pltpu.make_async_copy(w_ref.at[pl.ds(i * zt, zt)], wv.at[pl.ds(i * zt, zt)], in_sem.at[i])

    def qload(i):
        return pltpu.make_async_copy(q_ref.at[i], qv.at[i], q_sem.at[i])

    def store(i):
        return pltpu.make_async_copy(ov.at[i], o_ref.at[:, pl.ds(i * zt, zt)], out_sem.at[i])

    @pl.loop(0, nz)
    def _(i):
        qload(i).start()
        load(i).start()

    @pl.loop(0, nz)
    def _(i):
        qload(i).wait()
        load(i).wait()
        for z in range(0, zt, 2):
            hi, mid, lo = _split(_cat([src[pl.ds(i * k * zt + z + j, k, stride=zt), :] for j in range(2)]))
            rhs = jnp.concatenate([s.astype(F32) for s in (lo, mid, hi, mid, hi, hi)], axis=0).astype(BF16)
            out = jnp.dot(t_ref[...], rhs, preferred_element_type=F32)
            for j in range(2):
                dst[pl.ds(i * x * zt + z + j, x, stride=zt), :] = wv[i * zt + z + j] + out[:, j * y:(j + 1) * y]
        store(i).start()

    @pl.loop(0, nz)
    def _(i):
        store(i).wait()


def solution(mesh):
    na, nb = mesh.shape["a"], mesh.shape["b"]

    def local(u, g):
        n, ya, zb = u.shape
        nkx = g.shape[0]
        kx = nkx * na
        nchunk, npiece, nz = nkx // KC, nkx // KA, zb // ZT
        brows = (nchunk - NLAST) * 4 * KC
        tf, ti = _xforward(n, kx, na), _xinverse(n, kx, na)
        bulk = np.ascontiguousarray(ti[:, :brows])
        hi, mid, lo = _nsplit(ti[:, brows:])
        last = np.concatenate([hi, mid, lo, hi, mid, hi], axis=1)
        wy, wi = _ytables(n, nb)
        c, s = _trig(n, n, n)
        cs = np.concatenate([c, s]).astype(np.float32)
        ut = jnp.transpose(u, (0, 2, 1))
        anyspec = pl.BlockSpec(memory_space=pl.ANY)
        dma = pltpu.SemaphoreType.DMA
        vm = lambda *shape: pltpu.VMEM(shape, F32)
        acc, ql = pl.pallas_call(
            functools.partial(_spectral, nb), name="spectral",
            in_specs=[anyspec] * 7, out_specs=[anyspec] * 2,
            out_shape=[jax.ShapeDtypeStruct((zb, n, ya), F32),
                       jax.ShapeDtypeStruct((nz, NLAST, na, 2 * KC, ZT, ya), F32)],
            scratch_shapes=[
                vm(3, n, ZT, ya), vm(nz, na, ROWS, ZT, ya), vm(nz, ROWS, ZT, ya),
                vm(nkx, nb, zb, 128), vm(nkx, n, 128), vm(nkx, nb, zb, 128),
                vm(nz, nchunk, na, 2 * KC, ZT, ya), vm(2, ZT, n, ya), vm(2, KC, *g.shape[1:]),
                vm(*tf.shape), vm(*wy.shape), vm(*cs.shape), vm(*bulk.shape),
                pltpu.VMEM((3, *tf.shape), BF16), pltpu.VMEM((3, *wy.shape), BF16), pltpu.VMEM((3, *wi.shape), BF16),
                dma((5,)), dma((3,)), dma((2,)), dma((nz,)), dma((nz,)), dma((3, npiece)), dma((3, npiece)),
                dma((3, nchunk)), dma((3, nchunk)), dma((3, nchunk)), dma((3, nchunk)),
                dma((nchunk,)), dma((nchunk,)), dma((NLAST,)), dma((2,)),
            ],
            compiler_params=pltpu.CompilerParams(
                collective_id=0, has_side_effects=True, vmem_limit_bytes=67043328),
        )(ut, g, tf, wy, cs, wi, bulk)
        k = NLAST * na * 2 * KC
        w = pl.pallas_call(
            _finish, name="finish",
            in_specs=[pl.BlockSpec(memory_space=pltpu.VMEM), anyspec, anyspec], out_specs=anyspec,
            out_shape=jax.ShapeDtypeStruct((n, zb, ya), F32),
            scratch_shapes=[vm(zb, n, ya), vm(nz, k, ZT, ya), vm(nz, n, ZT, ya), dma((nz,)), dma((nz,)), dma((nz,))],
            compiler_params=pltpu.CompilerParams(vmem_limit_bytes=62 << 20),
        )(last, acc, ql.reshape(nz, k, ZT, ya))
        return jnp.transpose(w, (0, 2, 1))

    return jax.shard_map(local, mesh=mesh, in_specs=(P(None, "a", "b"), P("a", "b", None)), out_specs=P(None, "a", "b"), check_vma=False)
```

```python
import functools
import math
import jax
import jax.numpy as jnp
import numpy as np
from jax import lax
from jax.experimental import pallas as pl
from jax.experimental.pallas import tpu as pltpu
from jax.sharding import PartitionSpec as P

HI = lax.Precision.HIGHEST
F32, BF16 = jnp.float32, jnp.bfloat16
MESH = pl.DeviceIdType.MESH
KC = 5
KA = 13
NLAST = 2
ZT = 8
ROWS = 136
HALF = ROWS // 2
TROWS = 144
NA = 2


def _trig(n, rows, cols):
    r = np.arange(rows)[:, None]
    c = np.arange(cols)[None, :]
    ang = ((r * c) % n).astype(np.float32) * np.float32(2.0 * math.pi / n)
    return np.cos(ang.astype(np.float64)), np.sin(ang.astype(np.float64))


def _xforward(n, kx, na):
    cx, sx = _trig(n, kx, n)
    keep = (np.arange(kx) <= n // 2).astype(np.float64)[:, None]
    t = np.zeros((na, 2, HALF, n))
    t[:, 0, : kx // na] = (cx * keep).reshape(na, kx // na, n)
    t[:, 1, : kx // na] = (-sx * keep).reshape(na, kx // na, n)
    t = np.pad(t.reshape(na, ROWS, n), ((0, 0), (0, TROWS - ROWS), (0, 0)))
    return np.concatenate([t, t[:1]]).reshape((na + 1) * TROWS, n).astype(np.float32)


def _xinverse(n, kx, na):
    cx, sx = _trig(n, kx, n)
    k = np.arange(kx)
    wgt = (np.where((k == 0) | (k == n // 2), 1.0, 2.0) * (k <= n // 2) / n)[:, None]
    t = np.stack([cx * wgt, -sx * wgt], 1).reshape(na, kx // na // KC, KC, 2, n)
    return t.transpose(1, 0, 2, 3, 4).reshape(2 * kx, n).T.astype(np.float32).copy()


def _ytables(n, nb):
    c, s = _trig(n, n, n)
    full = np.block([[c, -s], [s, c]])
    w = full.reshape(2 * n, 2, nb, n // nb).transpose(0, 2, 1, 3).reshape(2 * n, 2 * n)
    inv = (full.T / n).reshape(2, nb, n // nb, 2 * n).transpose(1, 0, 2, 3)
    inv = inv.reshape(2 * n, 2, 2, n // 2).transpose(0, 2, 1, 3).reshape(2 * n, 2 * n)
    return w.astype(np.float32), inv.astype(np.float32)


def _split(x):
    hi = x.astype(BF16)
    x = x - hi.astype(F32)
    mid = x.astype(BF16)
    return hi, mid, (x - mid.astype(F32)).astype(BF16)


def _nsplit(x):
    hi = x.astype(jnp.bfloat16)
    x = x - hi.astype(np.float32)
    mid = x.astype(jnp.bfloat16)
    return hi, mid, (x - mid.astype(np.float32)).astype(jnp.bfloat16)


def _mm(p, q):
    d = functools.partial(jnp.dot, preferred_element_type=F32)
    return d(p[0], q[2]) + d(p[1], q[1]) + d(p[2], q[0]) + d(p[0], q[1]) + d(p[1], q[0]) + d(p[0], q[0])


def _dot(p, q):
    return jnp.dot(p, q, precision=HI, preferred_element_type=F32)


def _cat(parts):
    return jnp.concatenate(parts, axis=1)


def _spectral(nb, u_ref, g_ref, t_ref, wy_ref, cs_ref, wi_ref, ai_ref, acc_ref, ql_ref,
              uv, xb, ps, sf, r, v, gv, tv, wv, csv, aiv, tsp, wysp, wisp,
              load_sem, u_sem, g_sem, xa_send, xa_recv, fa_send, fa_recv, f_send, f_recv,
              b_send, b_recv, q_send, q_recv):
    b, a = lax.axis_index("b"), lax.axis_index("a")
    other = 1 - a
    nkx = g_ref.shape[0]
    nchunk, npiece = nkx // KC, nkx // KA
    nbulk = nchunk - NLAST
    n = r.shape[1]
    zb = n // nb
    nz = zb // ZT
    y = 128
    za, zr = NA * ZT, zb - NA * ZT
    npad = 2 * nkx - n // 2 - 1
    bx, by = lax.rem(b, 2), lax.div(b, 2)
    peers = [lax.rem(by + d // 2, 2) * 2 + lax.rem(bx + d % 2, 2) for d in (1, 2, 3)]
    us = uv.shape[0]

    def ck(i):
        return pl.ds(i * KC, KC)

    def ka(i):
        return pl.ds(i * KA, KA)

    loads = [pltpu.make_async_copy(s, d, load_sem.at[i]) for i, (s, d) in enumerate(
        [(t_ref, tv), (wy_ref, wv), (wi_ref, wv), (cs_ref, csv), (ai_ref, aiv)])]
    gs = gv.shape[0]

    def gload(i):
        return pltpu.make_async_copy(g_ref.at[ck(i)], gv.at[lax.rem(i, gs)], g_sem.at[lax.rem(i, gs)])

    def uload(z):
        return pltpu.make_async_copy(
            u_ref.at[:, pl.ds(z * ZT, ZT)], uv.at[lax.rem(z, us)], u_sem.at[lax.rem(z, us)])

    def xremote(z):
        return pltpu.make_async_remote_copy(
            ps.at[z], xb.at[z, a], xa_send.at[z], xa_recv.at[z], device_id=(b, other), device_id_type=MESH)

    def fwda(e, i, d, k):
        rows = pl.ds(i * KA, k)
        return pltpu.make_async_remote_copy(
            sf.at[rows, peers[d], pl.ds(e * ZT, ZT)], r.at[rows, pl.ds(b * zb + e * ZT, ZT)],
            fa_send.at[d, e * npiece + i], fa_recv.at[d, e * npiece + i],
            device_id=(peers[d], a), device_id_type=MESH)

    def fwd(i, d, k):
        rows = pl.ds(i * KC, k)
        return pltpu.make_async_remote_copy(
            sf.at[rows, peers[d], pl.ds(za, zr)], r.at[rows, pl.ds(b * zb + za, zr)],
            f_send.at[d, i], f_recv.at[d, i], device_id=(peers[d], a), device_id_type=MESH)

    def bwd(i, d, k):
        rows = pl.ds(i * KC, k)
        return pltpu.make_async_remote_copy(
            r.at[rows, pl.ds(peers[d] * zb, zb)], v.at[rows, b], b_send.at[d, i], b_recv.at[d, i],
            device_id=(peers[d], a), device_id_type=MESH)

    def sized(short, full, act):
        @pl.when(jnp.logical_not(short))
        def _():
            act(full)

        @pl.when(short)
        def _():
            act(full - npad)

    def each(i, full, last, act):
        sized(jnp.logical_and(i == last, a == 1), full, lambda k: [act(d, k) for d in range(3)])

    def eacha(i, act):
        each(i, KA, npiece - 1, act)

    def eachc(i, act):
        each(i, KC, nchunk - 1, act)

    def qsrc(i):
        return ps.at[:, pl.ds(i * 2 * KC, 2 * KC)]

    def qremote(i):
        return pltpu.make_async_remote_copy(
            qsrc(i), acc_ref.at[:, pl.ds((i * 2 + a) * 2 * KC, 2 * KC)], q_send.at[i], q_recv.at[i],
            device_id=(b, other), device_id_type=MESH)

    def qlast(i):
        return pltpu.make_async_remote_copy(
            qsrc(i), ql_ref.at[:, pl.ds(((i - nbulk) * 2 + a) * 2 * KC, 2 * KC)], q_send.at[i], q_recv.at[i],
            device_id=(b, other), device_id_type=MESH)

    barrier = pltpu.get_barrier_semaphore()
    for dev in [(b, other)] + [(pb, a) for pb in peers]:
        pl.semaphore_signal(barrier, inc=1, device_id=dev, device_id_type=MESH)
    loads[0].start()
    for z in range(us):
        uload(z).start()
    for c in (loads[1], loads[3], loads[4]):
        c.start()
    for i in range(gs):
        gload(i).start()

    src = uv.reshape(us * n * ZT, y)
    own = xb.reshape(nz * 2 * ROWS * ZT, y)
    sent = ps.reshape(nz * ROWS * ZT, y)

    def split_table(dst, step):
        @pl.loop(0, wv.shape[0] // step)
        def _(i):
            rows = pl.ds(i * step, step)
            for m, part in enumerate(_split(wv[rows, :])):
                dst[m, rows, :] = part

    def xhalf(zi, z, rhs, first, dst, base):
        rows = pl.ds(pl.multiple_of(first * TROWS, 16), TROWS)
        out = _mm([tsp[m, rows, :] for m in range(3)], rhs)
        for i in range(2):
            dst[pl.ds(base * ROWS * ZT + z + i, ROWS, stride=ZT), :] = out[:ROWS, i * y:(i + 1) * y]

    def xblock(zi, halves):
        slot = lax.rem(zi, us)
        for z in range(0, ZT, 2):
            rhs = _split(_cat([src[pl.ds(slot * n * ZT + z + i, n, stride=ZT), :] for i in range(2)]))
            if 1 in halves:
                xhalf(zi, z, rhs, a + 1, sent, zi)
            if 0 in halves:
                xhalf(zi, z, rhs, a, own, zi * 2 + a)

    loads[0].wait()
    for m, part in enumerate(_split(tv[...])):
        tsp[m] = part
    uload(0).wait()
    xblock(0, (1,))
    pl.semaphore_wait(barrier, 4)
    xremote(0).start()
    xblock(0, (0,))
    loads[1].wait()
    split_table(wysp, 128)
    loads[2].start()

    @pl.loop(0, NA)
    def _(e):
        xremote(e).wait_recv()

        @pl.loop(0, npiece)
        def _(i):
            x = _split(_cat([xb[e, h, pl.ds(c * HALF + i * KA, KA)].reshape(KA * ZT, y)
                             for c in range(2) for h in range(2)]))
            out = _mm(x, [wysp[m] for m in range(3)])
            zrow = pl.multiple_of(e * ZT, ZT)
            for k in range(nb):
                sf[ka(i), k, pl.ds(zrow, ZT)] = out[:, k * y:(k + 1) * y].reshape(KA, ZT, y)
            r[ka(i), pl.ds(b * zb + zrow, ZT)] = sf[ka(i), b, pl.ds(zrow, ZT)]
            eacha(i, lambda d, k: fwda(e, i, d, k).start())

        @pl.loop(1 + 2 * e, 3 + (nz - 3) * e)
        def _(z):
            @pl.when(z + us - 1 < nz)
            def _():
                uload(z + us - 1).start()
            uload(z).wait()
            xblock(z, (1, 0))
            xremote(z).start()

    @pl.loop(NA, nz)
    def _(z):
        xremote(z).wait_recv()

    @pl.loop(0, nchunk)
    def _(i):
        x = _cat([jnp.concatenate([xb[pl.ds(NA, nz - NA), h, c * HALF + i * KC + j].reshape(zr, y) for j in range(KC)])
                  for c in range(2) for h in range(2)])
        out = _mm(_split(x), [wysp[m] for m in range(3)])
        for k in range(nb):
            sf[ck(i), k, pl.ds(za, zr)] = out[:, k * y:(k + 1) * y].reshape(KC, zr, y)
        r[ck(i), pl.ds(b * zb + za, zr)] = sf[ck(i), b, pl.ds(za, zr)]
        eachc(i, lambda d, k: fwd(i, d, k).start())

    @pl.when(a == 1)
    def _():
        for k in range(npad):
            r[nkx - 1 - k] = jnp.zeros((n, y), F32)
            v[nkx - 1 - k] = jnp.zeros((nb, zb, y), F32)

    for c in loads[2:]:
        c.wait()
    split_table(wisp, 128)
    lane = lax.broadcasted_iota(jnp.int32, (n, y), 1)
    sign = jnp.where(lane < y // 2, 1.0, -1.0).astype(F32)

    @pl.loop(0, NA)
    def _(e):
        @pl.loop(0, npiece)
        def _(i):
            eacha(i, lambda d, k: fwda(e, i, d, k).wait_recv())

    @pl.loop(0, nchunk)
    def _(i):
        eachc(i, lambda d, k: fwd(i, d, k).wait_recv())
        gload(i).wait()
        e = _dot(csv[...], _cat([r[i * KC + j] for j in range(KC)]))
        parts = []
        for j in range(KC):
            cols = slice(j * y, (j + 1) * y)
            g1 = gv[lax.rem(i, gs), j] * (1.0 / n)
            gt = jnp.transpose(jnp.concatenate([g1, g1], axis=0))
            parts.append((e[:n, cols] + sign * pltpu.roll(e[n:, cols], y // 2, 1)) * gt)

        @pl.when(i + gs < nchunk)
        def _():
            gload(i + gs).start()
        e = _dot(csv[...], _cat(parts))
        for j in range(KC):
            cols = slice(j * y, (j + 1) * y)
            r[i * KC + j] = e[:n, cols] - sign * pltpu.roll(e[n:, cols], y // 2, 1)
        v[ck(i), b] = r[ck(i), pl.ds(b * zb, zb)]
        eachc(i, lambda d, k: bwd(i, d, k).start())

    @pl.loop(0, nz)
    def _(z):
        xremote(z).wait_send()

    def yinverse(i, own_ref, row):
        eachc(i, lambda d, k: bwd(i, d, k).wait_recv())
        out = _mm(_split(_cat([v[ck(i), k].reshape(KC * zb, y) for k in range(nb)])), [wisp[m] for m in range(3)])

        def tile(h, c, j):
            m = h * 2 + c
            return out[j * zb:(j + 1) * zb, m * y:(m + 1) * y].reshape(nz, ZT, y)

        for c in range(2):
            for j in range(KC):
                t0, t1 = tile(0, c, j), tile(1, c, j)
                own_ref[:, row + j * 2 + c] = jnp.where(a == 0, t0, t1)
                ps[:, i * 2 * KC + j * 2 + c] = jnp.where(a == 0, t1, t0)

    @pl.loop(0, nbulk)
    def _(i):
        yinverse(i, acc_ref, (i * 2 + a) * 2 * KC)
        qremote(i).start()

    @pl.loop(0, nbulk)
    def _(i):
        qremote(i).wait_recv()

    brows = nbulk * 4 * KC
    arows = acc_ref.shape[1]
    flat = acc_ref.reshape(nz * arows * ZT, y)

    @pl.loop(0, nz)
    def _(zi):
        for z in range(0, ZT, 2):
            rhs = _cat([flat[pl.ds(zi * arows * ZT + z + i, brows, stride=ZT), :] for i in range(2)])
            out = _dot(aiv[...], rhs)
            for i in range(2):
                flat[pl.ds(zi * arows * ZT + z + i, arows, stride=ZT), :] = out[:, i * y:(i + 1) * y]

    @pl.loop(nbulk, nchunk)
    def _(i):
        yinverse(i, ql_ref, ((i - nbulk) * 2 + a) * 2 * KC)
        qlast(i).start()

    @pl.loop(0, NA)
    def _(e):
        @pl.loop(0, npiece)
        def _(i):
            eacha(i, lambda d, k: fwda(e, i, d, k).wait_send())

    @pl.loop(0, nchunk)
    def _(i):
        eachc(i, lambda d, k: (fwd(i, d, k).wait_send(), bwd(i, d, k).wait_send()))

    @pl.loop(0, nbulk)
    def _(i):
        qremote(i).wait_send()

    @pl.loop(nbulk, nchunk)
    def _(i):
        qlast(i).wait()


def _finish(t_ref, w_ref, q_ref, o_ref, ov, out_sem):
    nz, x, zt, y = ov.shape
    k = q_ref.shape[1]
    src = q_ref.reshape(nz * k * zt, y)
    acc = w_ref.reshape(nz * x * zt, y)
    dst = ov.reshape(nz * x * zt, y)

    def store(i):
        return pltpu.make_async_copy(ov.at[i], o_ref.at[:, pl.ds(i * zt, zt)], out_sem.at[i])

    @pl.loop(0, nz)
    def _(i):
        for z in range(0, zt, 2):
            hi, mid, lo = _split(_cat([src[pl.ds(i * k * zt + z + j, k, stride=zt), :] for j in range(2)]))
            rhs = jnp.concatenate([s.astype(F32) for s in (lo, mid, hi, mid, hi, hi)], axis=0).astype(BF16)
            out = jnp.dot(t_ref[...], rhs, preferred_element_type=F32)
            for j in range(2):
                rows = pl.ds(i * x * zt + z + j, x, stride=zt)
                dst[rows, :] = acc[rows, :] + out[:, j * y:(j + 1) * y]
        store(i).start()

    @pl.loop(0, nz)
    def _(i):
        store(i).wait()


def solution(mesh):
    na, nb = mesh.shape["a"], mesh.shape["b"]

    def local(u, g):
        n, ya, zb = u.shape
        nkx = g.shape[0]
        kx = nkx * na
        nchunk, npiece, nz = nkx // KC, nkx // KA, zb // ZT
        klast = NLAST * na * 2 * KC
        brows = (nchunk - NLAST) * 4 * KC
        tf, ti = _xforward(n, kx, na), _xinverse(n, kx, na)
        bulk = np.ascontiguousarray(ti[:, :brows])
        hi, mid, lo = _nsplit(ti[:, brows:])
        last = np.concatenate([hi, mid, lo, hi, mid, hi], axis=1)
        wy, wi = _ytables(n, nb)
        c, s = _trig(n, n, n)
        cs = np.concatenate([c, s]).astype(np.float32)
        ut = jnp.transpose(u, (0, 2, 1))
        anyspec = pl.BlockSpec(memory_space=pl.ANY)
        vmspec = pl.BlockSpec(memory_space=pltpu.VMEM)
        dma = pltpu.SemaphoreType.DMA
        vm = lambda *shape: pltpu.VMEM(shape, F32)
        acc, ql = pl.pallas_call(
            functools.partial(_spectral, nb), name="spectral",
            in_specs=[pl.BlockSpec(memory_space=pltpu.HBM)] * 7, out_specs=[vmspec] * 2,
            out_shape=[vm(nz, n, ZT, ya), vm(nz, klast, ZT, ya)],
            scratch_shapes=[
                vm(3, n, ZT, ya), vm(nz, na, ROWS, ZT, ya), vm(nz, ROWS, ZT, ya),
                vm(nkx, nb, zb, 128), vm(nkx, n, 128), vm(nkx, nb, zb, 128),
                vm(2, KC, *g.shape[1:]),
                vm(*tf.shape), vm(*wy.shape), vm(*cs.shape), vm(*bulk.shape),
                pltpu.VMEM((3, *tf.shape), BF16), pltpu.VMEM((3, *wy.shape), BF16), pltpu.VMEM((3, *wi.shape), BF16),
                dma((5,)), dma((3,)), dma((2,)), dma((nz,)), dma((nz,)), dma((3, NA * npiece)), dma((3, NA * npiece)),
                dma((3, nchunk)), dma((3, nchunk)), dma((3, nchunk)), dma((3, nchunk)),
                dma((nchunk,)), dma((nchunk,)),
            ],
            compiler_params=pltpu.CompilerParams(
                collective_id=0, has_side_effects=True, vmem_limit_bytes=52 << 20),
        )(ut, g, tf, wy, cs, wi, bulk)
        w = pl.pallas_call(
            _finish, name="finish",
            in_specs=[vmspec] * 3, out_specs=anyspec,
            out_shape=jax.ShapeDtypeStruct((n, zb, ya), F32),
            scratch_shapes=[vm(nz, n, ZT, ya), dma((nz,))],
            compiler_params=pltpu.CompilerParams(vmem_limit_bytes=24 << 20),
        )(last, acc, ql)
        return jnp.transpose(w, (0, 2, 1))

    return jax.shard_map(local, mesh=mesh, in_specs=(P(None, "a", "b"), P("a", "b", None)), out_specs=P(None, "a", "b"), check_vma=False)
```

```python
import functools
import math
import jax
import jax.numpy as jnp
import numpy as np
from jax import lax
from jax.experimental import pallas as pl
from jax.experimental.pallas import tpu as pltpu
from jax.sharding import PartitionSpec as P

HI = lax.Precision.HIGHEST
F32, BF16 = jnp.float32, jnp.bfloat16
MESH = pl.DeviceIdType.MESH
KC = 5
KA = 13
NLAST = 4
ZT = 8
ROWS = 136
TROWS = 144
NA = 2
NS = 2
SL = 8


def _trig(n, rows, cols):
    r = np.arange(rows)[:, None]
    c = np.arange(cols)[None, :]
    ang = ((r * c) % n).astype(np.float32) * np.float32(2.0 * math.pi / n)
    return np.cos(ang.astype(np.float64)), np.sin(ang.astype(np.float64))


def _xforward(n, kx, na):
    cx, sx = _trig(n, kx, n)
    keep = (np.arange(kx) <= n // 2).astype(np.float64)[:, None]
    t = np.stack([cx * keep, -sx * keep]).reshape(2, na, -1, KA, n).transpose(1, 2, 0, 3, 4).reshape(na, -1, n)
    t = np.pad(t, ((0, 0), (0, TROWS - t.shape[1]), (0, 0)))
    return np.concatenate([t, t[:1]]).reshape((na + 1) * TROWS, n).astype(np.float32)


def _xinverse(n, kx, na):
    cx, sx = _trig(n, kx, n)
    k = np.arange(kx)
    wgt = (np.where((k == 0) | (k == n // 2), 1.0, 2.0) * (k <= n // 2) / n)[:, None]
    t = np.stack([cx * wgt, -sx * wgt], 1).reshape(na, kx // na, 2 * n)
    ends = list(range(0, kx // na - NS * KC + 1, KC)) + [kx // na]
    t = np.concatenate([t[:, i:j].reshape(-1, n) for i, j in zip(ends, ends[1:])])
    return t.T.astype(np.float32).copy()


def _ytables(n, nb):
    c, s = _trig(n, n, n)
    full = np.block([[c, -s], [s, c]])
    w = full.reshape(2 * n, 2, nb, n // nb).transpose(0, 2, 1, 3).reshape(2 * n, 2 * n)
    inv = (full.T / n).reshape(2, nb, n // nb, 2 * n).transpose(1, 0, 2, 3)
    inv = inv.reshape(2 * n, 2, 2, n // 2).transpose(0, 2, 1, 3).reshape(2 * n, 2 * n)
    return w.astype(np.float32), inv.astype(np.float32)


def _split(x):
    hi = x.astype(BF16)
    x = x - hi.astype(F32)
    mid = x.astype(BF16)
    return hi, mid, (x - mid.astype(F32)).astype(BF16)


def _nsplit(x):
    hi = x.astype(jnp.bfloat16)
    x = x - hi.astype(np.float32)
    mid = x.astype(jnp.bfloat16)
    return hi, mid, (x - mid.astype(np.float32)).astype(jnp.bfloat16)


def _mm(p, q):
    d = functools.partial(jnp.dot, preferred_element_type=F32)
    return d(p[0], q[2]) + d(p[1], q[1]) + d(p[2], q[0]) + d(p[0], q[1]) + d(p[1], q[0]) + d(p[0], q[0])


def _dot(p, q):
    return jnp.dot(p, q, precision=HI, preferred_element_type=F32)


def _cat(parts):
    return jnp.concatenate(parts, axis=1)


def _add_last(t_ref, q_ref, qrow, k, acc_ref, row, dst_ref, drow, x):
    for z in range(0, ZT, 2):
        hi, mid, lo = _split(_cat([q_ref[pl.ds(qrow + z + j, k, stride=ZT), :] for j in range(2)]))
        rhs = jnp.concatenate([s.astype(F32) for s in (lo, mid, hi, mid, hi, hi)], axis=0).astype(BF16)
        out = jnp.dot(t_ref[...], rhs, preferred_element_type=F32)
        for j in range(2):
            part = acc_ref[pl.ds(row + z + j, x, stride=ZT), :] + out[:, j * 128:(j + 1) * 128]
            dst_ref[pl.ds(drow + z + j, x, stride=ZT), :] = part


def _spectral(nb, u_ref, g_ref, t_ref, wy_ref, cs_ref, wi_ref, ai_ref, al_ref, acc_ref, ql_ref,
              uv, xb, ps, sf, r, v, gv, tv, wv, csv, aiv, tsp, wysp, wisp, alv,
              load_sem, u_sem, g_sem, xa_send, xa_recv, fa_send, fa_recv, f_send, f_recv,
              b_send, b_recv, q_send, q_recv, xp_send, xp_recv):
    b, a = lax.axis_index("b"), lax.axis_index("a")
    other = 1 - a
    nkx = g_ref.shape[0]
    nchunk, npiece = nkx // KC, nkx // KA
    nbulk = nchunk - NLAST
    n = r.shape[1]
    zb = n // nb
    nz = zb // ZT
    y = 128
    za, zr = NA * ZT, zb - NA * ZT
    npad = 2 * nkx - n // 2 - 1
    bx, by = lax.rem(b, 2), lax.div(b, 2)
    peers = [lax.rem(by + d // 2, 2) * 2 + lax.rem(bx + d % 2, 2) for d in (1, 2, 3)]
    us = uv.shape[0]

    def ck(i):
        return pl.ds(i * KC, KC)

    def ka(i):
        return pl.ds(i * KA, KA)

    loads = [pltpu.make_async_copy(s, d, load_sem.at[i]) for i, (s, d) in enumerate(
        [(t_ref, tv), (wy_ref, wv), (wi_ref, wv), (cs_ref, csv), (ai_ref, aiv), (al_ref, alv)])]
    gs = gv.shape[0]

    def gload(i):
        return pltpu.make_async_copy(g_ref.at[ck(i)], gv.at[lax.rem(i, gs)], g_sem.at[lax.rem(i, gs)])

    def uload(z):
        return pltpu.make_async_copy(
            u_ref.at[:, pl.ds(z * ZT, ZT)], uv.at[lax.rem(z, us)], u_sem.at[lax.rem(z, us)])

    def xremote(z):
        return pltpu.make_async_remote_copy(
            ps.at[z], xb.at[z, a], xa_send.at[z], xa_recv.at[z], device_id=(b, other), device_id_type=MESH)

    def xpiece(i):
        rows = pl.ds(i * 2 * KA, 2 * KA)
        return pltpu.make_async_remote_copy(
            ps.at[0, rows], xb.at[0, a, rows], xp_send.at[i], xp_recv.at[i],
            device_id=(b, other), device_id_type=MESH)

    def fwda(e, i, d, k):
        rows = pl.ds(i * KA, k)
        return pltpu.make_async_remote_copy(
            sf.at[rows, peers[d], pl.ds(e * ZT, ZT)], r.at[rows, pl.ds(b * zb + e * ZT, ZT)],
            fa_send.at[d, e * npiece + i], fa_recv.at[d, e * npiece + i],
            device_id=(peers[d], a), device_id_type=MESH)

    def fwd(i, d, k):
        rows = pl.ds(i * KC, k)
        return pltpu.make_async_remote_copy(
            sf.at[rows, peers[d], pl.ds(za, zr)], r.at[rows, pl.ds(b * zb + za, zr)],
            f_send.at[d, i], f_recv.at[d, i], device_id=(peers[d], a), device_id_type=MESH)

    def bwd(i, d, k):
        rows = pl.ds(i * KC, k)
        return pltpu.make_async_remote_copy(
            r.at[rows, pl.ds(peers[d] * zb, zb)], v.at[rows, b], b_send.at[d, i], b_recv.at[d, i],
            device_id=(peers[d], a), device_id_type=MESH)

    zs, nzi = zb // SL, nz // SL
    nwhole, nk = nchunk - NS, NS * KC
    k0 = nkx - nk
    qlrow = (nwhole - nbulk) * 4 * KC + a * 2 * nk

    def bwdl(p, d, k):
        rows = pl.ds(k0, k)
        return pltpu.make_async_remote_copy(
            r.at[rows, pl.ds(peers[d] * zb + p * zs, zs)], v.at[rows, b, pl.ds(p * zs, zs)],
            b_send.at[d, nwhole + p], b_recv.at[d, nwhole + p],
            device_id=(peers[d], a), device_id_type=MESH)

    def sized(short, full, act):
        @pl.when(jnp.logical_not(short))
        def _():
            act(full)

        @pl.when(short)
        def _():
            act(full - npad)

    def each(i, full, last, act):
        sized(jnp.logical_and(i == last, a == 1), full, lambda k: [act(d, k) for d in range(3)])

    def eacha(i, act):
        each(i, KA, npiece - 1, act)

    def eachc(i, act):
        each(i, KC, nchunk - 1, act)

    def qsrc(i):
        return ps.at[:, pl.ds(i * 2 * KC, 2 * KC)]

    def qremote(i):
        return pltpu.make_async_remote_copy(
            qsrc(i), acc_ref.at[:, pl.ds((i * 2 + a) * 2 * KC, 2 * KC)], q_send.at[i], q_recv.at[i],
            device_id=(b, other), device_id_type=MESH)

    def qlast(i):
        rows = pl.ds(((i - nbulk) * 2 + a) * 2 * KC, 2 * KC)
        return pltpu.make_async_remote_copy(
            qsrc(i), ql_ref.at[:, rows], q_send.at[i], q_recv.at[i], device_id=(b, other), device_id_type=MESH)

    def qslice(p):
        zi = pl.ds(p * nzi, nzi)
        return pltpu.make_async_remote_copy(
            ps.at[zi, pl.ds(k0 * 2, nk * 2)], ql_ref.at[zi, pl.ds(qlrow, nk * 2)],
            q_send.at[nwhole + p], q_recv.at[nwhole + p], device_id=(b, other), device_id_type=MESH)

    barrier = pltpu.get_barrier_semaphore()
    for dev in [(b, other)] + [(pb, a) for pb in peers]:
        pl.semaphore_signal(barrier, inc=1, device_id=dev, device_id_type=MESH)
    uload(0).start()
    loads[0].start()
    loads[1].start()

    src = uv.reshape(us * n * ZT, y)
    own = xb.reshape(nz * 2 * ROWS * ZT, y)
    sent = ps.reshape(nz * ROWS * ZT, y)

    def split_table(dst, step):
        @pl.loop(0, wv.shape[0] // step)
        def _(i):
            rows = pl.ds(i * step, step)
            for m, part in enumerate(_split(wv[rows, :])):
                dst[m, rows, :] = part

    def xhalf(zi, z, rhs, first, dst, base):
        rows = pl.ds(pl.multiple_of(first * TROWS, 16), TROWS)
        out = _mm([tsp[m, rows, :] for m in range(3)], rhs)
        for i in range(2):
            dst[pl.ds(base * ROWS * ZT + z + i, ROWS, stride=ZT), :] = out[:ROWS, i * y:(i + 1) * y]

    def xblock(zi, halves):
        slot = lax.rem(zi, us)
        for z in range(0, ZT, 2):
            rhs = _split(_cat([src[pl.ds(slot * n * ZT + z + i, n, stride=ZT), :] for i in range(2)]))
            if 1 in halves:
                xhalf(zi, z, rhs, a + 1, sent, zi)
            if 0 in halves:
                xhalf(zi, z, rhs, a, own, zi * 2 + a)

    loads[0].wait()
    for m, part in enumerate(_split(tv[...])):
        tsp[m] = part
    uload(0).wait()
    for z in range(1, us):
        uload(z).start()
    for c in loads[3:]:
        c.start()
    for i in range(gs):
        gload(i).start()
    xblock(0, (1,))
    pl.semaphore_wait(barrier, 4)

    @pl.loop(0, npiece)
    def _(i):
        xpiece(i).start()

    xblock(0, (0,))
    loads[1].wait()
    split_table(wysp, 128)
    loads[2].start()

    @pl.loop(0, NA)
    def _(e):
        @pl.when(e > 0)
        def _():
            xremote(e).wait_recv()

        @pl.loop(0, npiece)
        def _(i):
            @pl.when(e == 0)
            def _():
                xpiece(i).wait_recv()
            x = _split(_cat([xb[e, h, pl.ds((2 * i + c) * KA, KA)].reshape(KA * ZT, y)
                             for c in range(2) for h in range(2)]))
            out = _mm(x, [wysp[m] for m in range(3)])
            zrow = pl.multiple_of(e * ZT, ZT)
            for k in range(nb):
                sf[ka(i), k, pl.ds(zrow, ZT)] = out[:, k * y:(k + 1) * y].reshape(KA, ZT, y)
            r[ka(i), pl.ds(b * zb + zrow, ZT)] = sf[ka(i), b, pl.ds(zrow, ZT)]
            eacha(i, lambda d, k: fwda(e, i, d, k).start())

        @pl.loop(1 + 2 * e, 3 + (nz - 3) * e)
        def _(z):
            @pl.when(z + us - 1 < nz)
            def _():
                uload(z + us - 1).start()
            uload(z).wait()
            xblock(z, (1, 0))
            xremote(z).start()

    @pl.loop(NA, nz)
    def _(z):
        xremote(z).wait_recv()

    def xrow(k, c):
        return (lax.div(k, KA) * 2 + c) * KA + lax.rem(k, KA)

    @pl.loop(0, nchunk)
    def _(i):
        x = _cat([jnp.concatenate([xb[pl.ds(NA, nz - NA), h, xrow(i * KC + j, c)].reshape(zr, y) for j in range(KC)])
                  for c in range(2) for h in range(2)])
        out = _mm(_split(x), [wysp[m] for m in range(3)])
        for k in range(nb):
            sf[ck(i), k, pl.ds(za, zr)] = out[:, k * y:(k + 1) * y].reshape(KC, zr, y)
        r[ck(i), pl.ds(b * zb + za, zr)] = sf[ck(i), b, pl.ds(za, zr)]
        eachc(i, lambda d, k: fwd(i, d, k).start())

    @pl.when(a == 1)
    def _():
        for k in range(npad):
            r[nkx - 1 - k] = jnp.zeros((n, y), F32)
            v[nkx - 1 - k] = jnp.zeros((nb, zb, y), F32)

    for c in loads[2:]:
        c.wait()
    split_table(wisp, 128)
    lane = lax.broadcasted_iota(jnp.int32, (n, y), 1)
    sign = jnp.where(lane < y // 2, 1.0, -1.0).astype(F32)

    @pl.loop(0, NA)
    def _(e):
        @pl.loop(0, npiece)
        def _(i):
            eacha(i, lambda d, k: fwda(e, i, d, k).wait_recv())

    @pl.loop(0, nchunk)
    def _(i):
        eachc(i, lambda d, k: fwd(i, d, k).wait_recv())
        gload(i).wait()
        e = _dot(csv[...], _cat([r[i * KC + j] for j in range(KC)]))
        parts = []
        for j in range(KC):
            cols = slice(j * y, (j + 1) * y)
            g1 = gv[lax.rem(i, gs), j] * (1.0 / n)
            gt = jnp.transpose(jnp.concatenate([g1, g1], axis=0))
            parts.append((e[:n, cols] + sign * pltpu.roll(e[n:, cols], y // 2, 1)) * gt)

        @pl.when(i + gs < nchunk)
        def _():
            gload(i + gs).start()
        e = _dot(csv[...], _cat(parts))
        for j in range(KC):
            cols = slice(j * y, (j + 1) * y)
            r[i * KC + j] = e[:n, cols] - sign * pltpu.roll(e[n:, cols], y // 2, 1)
        v[ck(i), b] = r[ck(i), pl.ds(b * zb, zb)]

        @pl.when(i < nwhole)
        def _():
            for d in range(3):
                bwd(i, d, KC).start()

    @pl.loop(0, SL)
    def _(p):
        sized(a == 1, nk, lambda k: [bwdl(p, d, k).start() for d in range(3)])

    @pl.loop(0, npiece)
    def _(i):
        xpiece(i).wait_send()

    @pl.loop(1, nz)
    def _(z):
        xremote(z).wait_send()

    def yinverse(k, nk, own_ref, row, p, zs):
        z0, nzi = pl.multiple_of(p * zs, ZT), zs // ZT
        zi = pl.ds(p * nzi, nzi)
        x = _cat([v[pl.ds(k, nk), m, pl.ds(z0, zs)].reshape(nk * zs, y) for m in range(nb)])
        out = _mm(_split(x), [wisp[m] for m in range(3)])

        def tile(h, c, j):
            m = h * 2 + c
            return out[j * zs:(j + 1) * zs, m * y:(m + 1) * y].reshape(nzi, ZT, y)

        for c in range(2):
            for j in range(nk):
                t0, t1 = tile(0, c, j), tile(1, c, j)
                own_ref[zi, row + j * 2 + c] = jnp.where(a == 0, t0, t1)
                ps[zi, k * 2 + j * 2 + c] = jnp.where(a == 0, t1, t0)

    @pl.loop(0, nbulk)
    def _(i):
        for d in range(3):
            bwd(i, d, KC).wait_recv()
        yinverse(i * KC, KC, acc_ref, (i * 2 + a) * 2 * KC, 0, zb)
        qremote(i).start()

    @pl.loop(0, nbulk)
    def _(i):
        qremote(i).wait_recv()

    brows = nbulk * 4 * KC
    arows = acc_ref.shape[1]
    flat = acc_ref.reshape(nz * arows * ZT, y)

    @pl.loop(0, nz)
    def _(zi):
        for z in range(0, ZT, 2):
            rhs = _cat([flat[pl.ds(zi * arows * ZT + z + i, brows, stride=ZT), :] for i in range(2)])
            out = _dot(aiv[...], rhs)
            for i in range(2):
                flat[pl.ds(zi * arows * ZT + z + i, arows, stride=ZT), :] = out[:, i * y:(i + 1) * y]

    @pl.loop(nbulk, nwhole)
    def _(i):
        for d in range(3):
            bwd(i, d, KC).wait_recv()
        yinverse(i * KC, KC, ql_ref, ((i - nbulk) * 2 + a) * 2 * KC, 0, zb)
        qlast(i).start()

    krows = ql_ref.shape[1]
    qflat = ql_ref.reshape(nz * krows * ZT, y)

    @pl.loop(nbulk, nwhole)
    def _(i):
        qlast(i).wait_recv()

    @pl.loop(0, SL)
    def _(p):
        sized(a == 1, nk, lambda k: [bwdl(p, d, k).wait_recv() for d in range(3)])
        yinverse(k0, nk, ql_ref, qlrow, p, zs)
        qslice(p).start()

        @pl.when(p > 0)
        def _():
            qslice(p - 1).wait_recv()

            @pl.loop((p - 1) * nzi, p * nzi)
            def _(zi):
                _add_last(alv, qflat, zi * krows * ZT, krows, flat, zi * arows * ZT, flat, zi * arows * ZT, arows)

    @pl.loop(0, NA)
    def _(e):
        @pl.loop(0, npiece)
        def _(i):
            eacha(i, lambda d, k: fwda(e, i, d, k).wait_send())

    @pl.loop(0, nchunk)
    def _(i):
        eachc(i, lambda d, k: fwd(i, d, k).wait_send())

    @pl.loop(0, nwhole)
    def _(i):
        for d in range(3):
            bwd(i, d, KC).wait_send()

    @pl.loop(0, nbulk)
    def _(i):
        qremote(i).wait_send()

    @pl.loop(nbulk, nwhole)
    def _(i):
        qlast(i).wait_send()

    @pl.loop(0, SL)
    def _(p):
        sized(a == 1, nk, lambda k: [bwdl(p, d, k).wait_send() for d in range(3)])
        qslice(p).wait_send()

    qslice(SL - 1).wait_recv()


def _finish(t_ref, w_ref, q_ref, o_ref, ov, out_sem):
    nz, x, zt, y = w_ref.shape
    k = q_ref.shape[1]
    rest = ov.shape[0]
    src = q_ref.reshape(nz * k * zt, y)
    acc = w_ref.reshape(nz * x * zt, y)
    dst = ov.reshape(rest * x * zt, y)

    def store(i, ref):
        return pltpu.make_async_copy(ref, o_ref.at[:, pl.ds(i * zt, zt)], out_sem.at[i])

    for i in range(nz - rest):
        store(i, w_ref.at[i]).start()
    for j in range(rest):
        i = nz - rest + j
        _add_last(t_ref, src, i * k * zt, k, acc, i * x * zt, dst, j * x * zt, x)
        store(i, ov.at[j]).start()
    for i in range(nz - rest):
        store(i, w_ref.at[i]).wait()
    for j in range(rest):
        store(nz - rest + j, ov.at[j]).wait()


def solution(mesh):
    na, nb = mesh.shape["a"], mesh.shape["b"]

    def local(u, g):
        n, ya, zb = u.shape
        nkx = g.shape[0]
        kx = nkx * na
        nchunk, npiece, nz = nkx // KC, nkx // KA, zb // ZT
        klast = NLAST * na * 2 * KC
        brows = (nchunk - NLAST) * 4 * KC
        tf, ti = _xforward(n, kx, na), _xinverse(n, kx, na)
        bulk = np.ascontiguousarray(ti[:, :brows])
        hi, mid, lo = _nsplit(ti[:, brows:])
        last = np.concatenate([hi, mid, lo, hi, mid, hi], axis=1)
        wy, wi = _ytables(n, nb)
        c, s = _trig(n, n, n)
        cs = np.concatenate([c, s]).astype(np.float32)
        ut = jnp.transpose(u, (0, 2, 1))
        anyspec = pl.BlockSpec(memory_space=pl.ANY)
        vmspec = pl.BlockSpec(memory_space=pltpu.VMEM)
        dma = pltpu.SemaphoreType.DMA
        vm = lambda *shape: pltpu.VMEM(shape, F32)
        acc, ql = pl.pallas_call(
            functools.partial(_spectral, nb), name="spectral",
            in_specs=[pl.BlockSpec(memory_space=pltpu.HBM)] * 8, out_specs=[vmspec] * 2,
            out_shape=[vm(nz, n, ZT, ya), vm(nz, klast, ZT, ya)],
            scratch_shapes=[
                vm(3, n, ZT, ya), vm(nz, na, ROWS, ZT, ya), vm(nz, ROWS, ZT, ya),
                vm(nkx, nb, zb, 128), vm(nkx, n, 128), vm(nkx, nb, zb, 128),
                vm(2, KC, *g.shape[1:]),
                vm(*tf.shape), vm(*wy.shape), vm(*cs.shape), vm(*bulk.shape),
                pltpu.VMEM((3, *tf.shape), BF16), pltpu.VMEM((3, *wy.shape), BF16), pltpu.VMEM((3, *wi.shape), BF16),
                pltpu.VMEM(last.shape, BF16),
                dma((6,)), dma((3,)), dma((2,)), dma((nz,)), dma((nz,)), dma((3, NA * npiece)), dma((3, NA * npiece)),
                dma((3, nchunk)), dma((3, nchunk)), dma((3, nchunk + SL)), dma((3, nchunk + SL)),
                dma((nchunk + SL,)), dma((nchunk + SL,)), dma((npiece,)), dma((npiece,)),
            ],
            compiler_params=pltpu.CompilerParams(
                collective_id=0, has_side_effects=True, vmem_limit_bytes=53 << 20),
        )(ut, g, tf, wy, cs, wi, bulk, last)
        w = pl.pallas_call(
            _finish, name="finish",
            in_specs=[vmspec] * 3, out_specs=anyspec,
            out_shape=jax.ShapeDtypeStruct((n, zb, ya), F32),
            scratch_shapes=[vm(nz // SL, n, ZT, ya), dma((nz,))],
            compiler_params=pltpu.CompilerParams(vmem_limit_bytes=24 << 20),
        )(last, acc, ql)
        return jnp.transpose(w, (0, 2, 1))

    return jax.shard_map(local, mesh=mesh, in_specs=(P(None, "a", "b"), P("a", "b", None)), out_specs=P(None, "a", "b"), check_vma=False)
```

```python
import functools
import math
import jax
import jax.numpy as jnp
import numpy as np
from jax import lax
from jax.experimental import pallas as pl
from jax.experimental.pallas import tpu as pltpu
from jax.sharding import PartitionSpec as P

HI = lax.Precision.HIGHEST
F32, BF16 = jnp.float32, jnp.bfloat16
MESH = pl.DeviceIdType.MESH
KC = 5
KA = 13
NLAST = 4
ZT = 8
ROWS = 136
TROWS = 144
NA = 2
NS = 3
SL = 8


def _trig(n, rows, cols):
    r = np.arange(rows)[:, None]
    c = np.arange(cols)[None, :]
    ang = ((r * c) % n).astype(np.float32) * np.float32(2.0 * math.pi / n)
    return np.cos(ang.astype(np.float64)), np.sin(ang.astype(np.float64))


def _xforward(n, kx, na):
    cx, sx = _trig(n, kx, n)
    keep = (np.arange(kx) <= n // 2).astype(np.float64)[:, None]
    t = np.stack([cx * keep, -sx * keep]).reshape(2, na, -1, KA, n).transpose(1, 2, 0, 3, 4).reshape(na, -1, n)
    t = np.pad(t, ((0, 0), (0, TROWS - t.shape[1]), (0, 0)))
    return np.concatenate([t, t[:1]]).reshape((na + 1) * TROWS, n).astype(np.float32)


def _xinverse(n, kx, na):
    cx, sx = _trig(n, kx, n)
    k = np.arange(kx)
    wgt = (np.where((k == 0) | (k == n // 2), 1.0, 2.0) * (k <= n // 2) / n)[:, None]
    t = np.stack([cx * wgt, -sx * wgt], 1).reshape(na, kx // na, 2 * n)
    ends = list(range(0, kx // na - NS * KC + 1, KC)) + [kx // na]
    t = np.concatenate([t[:, i:j].reshape(-1, n) for i, j in zip(ends, ends[1:])])
    return t.T.astype(np.float32).copy()


def _ytables(n, nb):
    c, s = _trig(n, n, n)
    full = np.block([[c, -s], [s, c]])
    w = full.reshape(2 * n, 2, nb, n // nb).transpose(0, 2, 1, 3).reshape(2 * n, 2 * n)
    inv = (full.T / n).reshape(2, nb, n // nb, 2 * n).transpose(1, 0, 2, 3)
    inv = inv.reshape(2 * n, 2, 2, n // 2).transpose(0, 2, 1, 3).reshape(2 * n, 2 * n)
    return w.astype(np.float32), inv.astype(np.float32)


def _split(x):
    hi = x.astype(BF16)
    x = x - hi.astype(F32)
    mid = x.astype(BF16)
    return hi, mid, (x - mid.astype(F32)).astype(BF16)


def _nsplit(x):
    hi = x.astype(jnp.bfloat16)
    x = x - hi.astype(np.float32)
    mid = x.astype(jnp.bfloat16)
    return hi, mid, (x - mid.astype(np.float32)).astype(jnp.bfloat16)


def _mm(p, q):
    d = functools.partial(jnp.dot, preferred_element_type=F32)
    return d(p[0], q[2]) + d(p[1], q[1]) + d(p[2], q[0]) + d(p[0], q[1]) + d(p[1], q[0]) + d(p[0], q[0])


def _dot(p, q):
    return jnp.dot(p, q, precision=HI, preferred_element_type=F32)


def _cat(parts):
    return jnp.concatenate(parts, axis=1)


def _add_last(t_ref, q_ref, qrow, k, acc_ref, row, dst_ref, drow, x):
    for z in range(0, ZT, 2):
        hi, mid, lo = _split(_cat([q_ref[pl.ds(qrow + z + j, k, stride=ZT), :] for j in range(2)]))
        rhs = jnp.concatenate([s.astype(F32) for s in (lo, mid, hi, mid, hi, hi)], axis=0).astype(BF16)
        out = jnp.dot(t_ref[...], rhs, preferred_element_type=F32)
        for j in range(2):
            part = acc_ref[pl.ds(row + z + j, x, stride=ZT), :] + out[:, j * 128:(j + 1) * 128]
            dst_ref[pl.ds(drow + z + j, x, stride=ZT), :] = part


def _spectral(nb, u_ref, g_ref, t_ref, wy_ref, cs_ref, wi_ref, ai_ref, al_ref, acc_ref, ql_ref,
              uv, xb, ps, sf, r, v, gv, tv, wv, csv, aiv, tsp, wysp, wisp, alv,
              load_sem, u_sem, g_sem, xa_send, xa_recv, fa_send, fa_recv, f_send, f_recv,
              b_send, b_recv, q_send, q_recv, xp_send, xp_recv):
    b, a = lax.axis_index("b"), lax.axis_index("a")
    other = 1 - a
    nkx = g_ref.shape[0]
    nchunk, npiece = nkx // KC, nkx // KA
    nbulk = nchunk - NLAST
    n = r.shape[1]
    zb = n // nb
    nz = zb // ZT
    y = 128
    za, zr = NA * ZT, zb - NA * ZT
    npad = 2 * nkx - n // 2 - 1
    bx, by = lax.rem(b, 2), lax.div(b, 2)
    peers = [lax.rem(by + d // 2, 2) * 2 + lax.rem(bx + d % 2, 2) for d in (1, 2, 3)]
    us = uv.shape[0]

    def ck(i):
        return pl.ds(i * KC, KC)

    def ka(i):
        return pl.ds(i * KA, KA)

    loads = [pltpu.make_async_copy(s, d, load_sem.at[i]) for i, (s, d) in enumerate(
        [(t_ref, tv), (wy_ref, wv), (wi_ref, wv), (cs_ref, csv), (ai_ref, aiv), (al_ref, alv)])]
    gs = gv.shape[0]

    def gload(i):
        return pltpu.make_async_copy(g_ref.at[ck(i)], gv.at[lax.rem(i, gs)], g_sem.at[lax.rem(i, gs)])

    def uload(z):
        return pltpu.make_async_copy(
            u_ref.at[:, pl.ds(z * ZT, ZT)], uv.at[lax.rem(z, us)], u_sem.at[lax.rem(z, us)])

    def xremote(z):
        return pltpu.make_async_remote_copy(
            ps.at[z], xb.at[z, a], xa_send.at[z], xa_recv.at[z], device_id=(b, other), device_id_type=MESH)

    def xpiece(i):
        rows = pl.ds(i * 2 * KA, 2 * KA)
        return pltpu.make_async_remote_copy(
            ps.at[0, rows], xb.at[0, a, rows], xp_send.at[i], xp_recv.at[i],
            device_id=(b, other), device_id_type=MESH)

    def fwda(e, i, d, k):
        rows = pl.ds(i * KA, k)
        return pltpu.make_async_remote_copy(
            sf.at[rows, peers[d], pl.ds(e * ZT, ZT)], r.at[rows, pl.ds(b * zb + e * ZT, ZT)],
            fa_send.at[d, e * npiece + i], fa_recv.at[d, e * npiece + i],
            device_id=(peers[d], a), device_id_type=MESH)

    def fwd(i, d, k):
        rows = pl.ds(i * KC, k)
        return pltpu.make_async_remote_copy(
            sf.at[rows, peers[d], pl.ds(za, zr)], r.at[rows, pl.ds(b * zb + za, zr)],
            f_send.at[d, i], f_recv.at[d, i], device_id=(peers[d], a), device_id_type=MESH)

    def bwd(i, d, k):
        rows = pl.ds(i * KC, k)
        return pltpu.make_async_remote_copy(
            r.at[rows, pl.ds(peers[d] * zb, zb)], v.at[rows, b], b_send.at[d, i], b_recv.at[d, i],
            device_id=(peers[d], a), device_id_type=MESH)

    zs, nzi = zb // SL, nz // SL
    nwhole, nk = nchunk - NS, NS * KC
    k0 = nkx - nk
    qlrow = (nwhole - nbulk) * 4 * KC + a * 2 * nk

    def bwdl(p, d, k):
        rows = pl.ds(k0, k)
        return pltpu.make_async_remote_copy(
            r.at[rows, pl.ds(peers[d] * zb + p * zs, zs)], v.at[rows, b, pl.ds(p * zs, zs)],
            b_send.at[d, nwhole + p], b_recv.at[d, nwhole + p],
            device_id=(peers[d], a), device_id_type=MESH)

    def sized(short, full, act):
        @pl.when(jnp.logical_not(short))
        def _():
            act(full)

        @pl.when(short)
        def _():
            act(full - npad)

    def each(i, full, last, act):
        sized(jnp.logical_and(i == last, a == 1), full, lambda k: [act(d, k) for d in range(3)])

    def eacha(i, act):
        each(i, KA, npiece - 1, act)

    def eachc(i, act):
        each(i, KC, nchunk - 1, act)

    def qsrc(i):
        return ps.at[:, pl.ds(i * 2 * KC, 2 * KC)]

    def qremote(i):
        return pltpu.make_async_remote_copy(
            qsrc(i), acc_ref.at[:, pl.ds((i * 2 + a) * 2 * KC, 2 * KC)], q_send.at[i], q_recv.at[i],
            device_id=(b, other), device_id_type=MESH)

    def qlast(i):
        rows = pl.ds(((i - nbulk) * 2 + a) * 2 * KC, 2 * KC)
        return pltpu.make_async_remote_copy(
            qsrc(i), ql_ref.at[:, rows], q_send.at[i], q_recv.at[i], device_id=(b, other), device_id_type=MESH)

    def qslice(p):
        zi = pl.ds(p * nzi, nzi)
        return pltpu.make_async_remote_copy(
            ps.at[zi, pl.ds(k0 * 2, nk * 2)], ql_ref.at[zi, pl.ds(qlrow, nk * 2)],
            q_send.at[nwhole + p], q_recv.at[nwhole + p], device_id=(b, other), device_id_type=MESH)

    barrier = pltpu.get_barrier_semaphore()
    for dev in [(b, other)] + [(pb, a) for pb in peers]:
        pl.semaphore_signal(barrier, inc=1, device_id=dev, device_id_type=MESH)
    uload(0).start()
    loads[0].start()
    loads[1].start()

    src = uv.reshape(us * n * ZT, y)
    own = xb.reshape(nz * 2 * ROWS * ZT, y)
    sent = ps.reshape(nz * ROWS * ZT, y)

    def split_table(dst, step):
        @pl.loop(0, wv.shape[0] // step)
        def _(i):
            rows = pl.ds(i * step, step)
            for m, part in enumerate(_split(wv[rows, :])):
                dst[m, rows, :] = part

    def xhalf(zi, z, rhs, first, dst, base):
        rows = pl.ds(pl.multiple_of(first * TROWS, 16), TROWS)
        out = _mm([tsp[m, rows, :] for m in range(3)], rhs)
        for i in range(2):
            dst[pl.ds(base * ROWS * ZT + z + i, ROWS, stride=ZT), :] = out[:ROWS, i * y:(i + 1) * y]

    def xblock(zi, halves):
        slot = lax.rem(zi, us)
        for z in range(0, ZT, 2):
            rhs = _split(_cat([src[pl.ds(slot * n * ZT + z + i, n, stride=ZT), :] for i in range(2)]))
            if 1 in halves:
                xhalf(zi, z, rhs, a + 1, sent, zi)
            if 0 in halves:
                xhalf(zi, z, rhs, a, own, zi * 2 + a)

    loads[0].wait()
    for m, part in enumerate(_split(tv[...])):
        tsp[m] = part
    uload(0).wait()
    for z in range(1, us):
        uload(z).start()
    for c in loads[3:]:
        c.start()
    for i in range(gs):
        gload(i).start()
    xblock(0, (1,))
    pl.semaphore_wait(barrier, 4)

    @pl.loop(0, npiece)
    def _(i):
        xpiece(i).start()

    xblock(0, (0,))
    loads[1].wait()
    split_table(wysp, 128)
    loads[2].start()

    @pl.loop(0, NA)
    def _(e):
        @pl.when(e > 0)
        def _():
            xremote(e).wait_recv()

        @pl.loop(0, npiece)
        def _(i):
            @pl.when(e == 0)
            def _():
                xpiece(i).wait_recv()
            x = _split(_cat([xb[e, h, pl.ds((2 * i + c) * KA, KA)].reshape(KA * ZT, y)
                             for c in range(2) for h in range(2)]))
            out = _mm(x, [wysp[m] for m in range(3)])
            zrow = pl.multiple_of(e * ZT, ZT)
            for k in range(nb):
                sf[ka(i), k, pl.ds(zrow, ZT)] = out[:, k * y:(k + 1) * y].reshape(KA, ZT, y)
            r[ka(i), pl.ds(b * zb + zrow, ZT)] = sf[ka(i), b, pl.ds(zrow, ZT)]
            eacha(i, lambda d, k: fwda(e, i, d, k).start())

        @pl.loop(1 + 2 * e, 3 + (nz - 3) * e)
        def _(z):
            @pl.when(z + us - 1 < nz)
            def _():
                uload(z + us - 1).start()
            uload(z).wait()
            xblock(z, (1, 0))
            xremote(z).start()

    @pl.loop(NA, nz)
    def _(z):
        xremote(z).wait_recv()

    def xrow(k, c):
        return (lax.div(k, KA) * 2 + c) * KA + lax.rem(k, KA)

    @pl.loop(0, nchunk)
    def _(i):
        x = _cat([jnp.concatenate([xb[pl.ds(NA, nz - NA), h, xrow(i * KC + j, c)].reshape(zr, y) for j in range(KC)])
                  for c in range(2) for h in range(2)])
        out = _mm(_split(x), [wysp[m] for m in range(3)])
        for k in range(nb):
            sf[ck(i), k, pl.ds(za, zr)] = out[:, k * y:(k + 1) * y].reshape(KC, zr, y)
        r[ck(i), pl.ds(b * zb + za, zr)] = sf[ck(i), b, pl.ds(za, zr)]
        eachc(i, lambda d, k: fwd(i, d, k).start())

    @pl.when(a == 1)
    def _():
        for k in range(npad):
            r[nkx - 1 - k] = jnp.zeros((n, y), F32)
            v[nkx - 1 - k] = jnp.zeros((nb, zb, y), F32)

    for c in loads[2:]:
        c.wait()
    split_table(wisp, 128)
    lane = lax.broadcasted_iota(jnp.int32, (n, y), 1)
    sign = jnp.where(lane < y // 2, 1.0, -1.0).astype(F32)

    @pl.loop(0, NA)
    def _(e):
        @pl.loop(0, npiece)
        def _(i):
            eacha(i, lambda d, k: fwda(e, i, d, k).wait_recv())

    @pl.loop(0, nchunk)
    def _(i):
        eachc(i, lambda d, k: fwd(i, d, k).wait_recv())
        gload(i).wait()
        e = _dot(csv[...], _cat([r[i * KC + j] for j in range(KC)]))
        parts = []
        for j in range(KC):
            cols = slice(j * y, (j + 1) * y)
            g1 = gv[lax.rem(i, gs), j] * (1.0 / n)
            gt = jnp.transpose(jnp.concatenate([g1, g1], axis=0))
            parts.append((e[:n, cols] + sign * pltpu.roll(e[n:, cols], y // 2, 1)) * gt)

        @pl.when(i + gs < nchunk)
        def _():
            gload(i + gs).start()
        e = _dot(csv[...], _cat(parts))
        for j in range(KC):
            cols = slice(j * y, (j + 1) * y)
            r[i * KC + j] = e[:n, cols] - sign * pltpu.roll(e[n:, cols], y // 2, 1)
        v[ck(i), b] = r[ck(i), pl.ds(b * zb, zb)]

        @pl.when(i < nwhole)
        def _():
            for d in range(3):
                bwd(i, d, KC).start()

    @pl.loop(0, SL)
    def _(p):
        sized(a == 1, nk, lambda k: [bwdl(p, d, k).start() for d in range(3)])

    @pl.loop(0, npiece)
    def _(i):
        xpiece(i).wait_send()

    @pl.loop(1, nz)
    def _(z):
        xremote(z).wait_send()

    def yinverse(k, nk, own_ref, row, p, zs):
        z0, nzi = pl.multiple_of(p * zs, ZT), zs // ZT
        zi = pl.ds(p * nzi, nzi)
        x = _cat([v[pl.ds(k, nk), m, pl.ds(z0, zs)].reshape(nk * zs, y) for m in range(nb)])
        out = _mm(_split(x), [wisp[m] for m in range(3)])

        def tile(h, c, j):
            m = h * 2 + c
            return out[j * zs:(j + 1) * zs, m * y:(m + 1) * y].reshape(nzi, ZT, y)

        for c in range(2):
            for j in range(nk):
                t0, t1 = tile(0, c, j), tile(1, c, j)
                own_ref[zi, row + j * 2 + c] = jnp.where(a == 0, t0, t1)
                ps[zi, k * 2 + j * 2 + c] = jnp.where(a == 0, t1, t0)

    @pl.loop(0, nbulk)
    def _(i):
        for d in range(3):
            bwd(i, d, KC).wait_recv()
        yinverse(i * KC, KC, acc_ref, (i * 2 + a) * 2 * KC, 0, zb)
        qremote(i).start()

    @pl.loop(0, nbulk)
    def _(i):
        qremote(i).wait_recv()

    brows = nbulk * 4 * KC
    arows = acc_ref.shape[1]
    flat = acc_ref.reshape(nz * arows * ZT, y)

    @pl.loop(0, nz)
    def _(zi):
        for z in range(0, ZT, 2):
            rhs = _cat([flat[pl.ds(zi * arows * ZT + z + i, brows, stride=ZT), :] for i in range(2)])
            out = _dot(aiv[...], rhs)
            for i in range(2):
                flat[pl.ds(zi * arows * ZT + z + i, arows, stride=ZT), :] = out[:, i * y:(i + 1) * y]

    @pl.loop(nbulk, nwhole)
    def _(i):
        for d in range(3):
            bwd(i, d, KC).wait_recv()
        yinverse(i * KC, KC, ql_ref, ((i - nbulk) * 2 + a) * 2 * KC, 0, zb)
        qlast(i).start()

    krows = ql_ref.shape[1]
    qflat = ql_ref.reshape(nz * krows * ZT, y)

    @pl.loop(nbulk, nwhole)
    def _(i):
        qlast(i).wait_recv()

    @pl.loop(0, SL)
    def _(p):
        sized(a == 1, nk, lambda k: [bwdl(p, d, k).wait_recv() for d in range(3)])
        yinverse(k0, nk, ql_ref, qlrow, p, zs)
        qslice(p).start()

        @pl.when(p > 0)
        def _():
            qslice(p - 1).wait_recv()

            @pl.loop((p - 1) * nzi, p * nzi)
            def _(zi):
                _add_last(alv, qflat, zi * krows * ZT, krows, flat, zi * arows * ZT, flat, zi * arows * ZT, arows)

    @pl.loop(0, NA)
    def _(e):
        @pl.loop(0, npiece)
        def _(i):
            eacha(i, lambda d, k: fwda(e, i, d, k).wait_send())

    @pl.loop(0, nchunk)
    def _(i):
        eachc(i, lambda d, k: fwd(i, d, k).wait_send())

    @pl.loop(0, nwhole)
    def _(i):
        for d in range(3):
            bwd(i, d, KC).wait_send()

    @pl.loop(0, nbulk)
    def _(i):
        qremote(i).wait_send()

    @pl.loop(nbulk, nwhole)
    def _(i):
        qlast(i).wait_send()

    @pl.loop(0, SL)
    def _(p):
        sized(a == 1, nk, lambda k: [bwdl(p, d, k).wait_send() for d in range(3)])
        qslice(p).wait_send()

    qslice(SL - 1).wait_recv()


def _finish(t_ref, w_ref, q_ref, o_ref, ov, out_sem):
    nz, x, zt, y = w_ref.shape
    k = q_ref.shape[1]
    rest = ov.shape[0]
    src = q_ref.reshape(nz * k * zt, y)
    acc = w_ref.reshape(nz * x * zt, y)
    dst = ov.reshape(rest * x * zt, y)

    def store(i, ref):
        return pltpu.make_async_copy(ref, o_ref.at[:, pl.ds(i * zt, zt)], out_sem.at[i])

    for i in range(nz - rest):
        store(i, w_ref.at[i]).start()
    for j in range(rest):
        i = nz - rest + j
        _add_last(t_ref, src, i * k * zt, k, acc, i * x * zt, dst, j * x * zt, x)
        store(i, ov.at[j]).start()
    for i in range(nz - rest):
        store(i, w_ref.at[i]).wait()
    for j in range(rest):
        store(nz - rest + j, ov.at[j]).wait()


def solution(mesh):
    na, nb = mesh.shape["a"], mesh.shape["b"]

    def local(u, g):
        n, ya, zb = u.shape
        nkx = g.shape[0]
        kx = nkx * na
        nchunk, npiece, nz = nkx // KC, nkx // KA, zb // ZT
        klast = NLAST * na * 2 * KC
        brows = (nchunk - NLAST) * 4 * KC
        tf, ti = _xforward(n, kx, na), _xinverse(n, kx, na)
        bulk = np.ascontiguousarray(ti[:, :brows])
        hi, mid, lo = _nsplit(ti[:, brows:])
        last = np.concatenate([hi, mid, lo, hi, mid, hi], axis=1)
        wy, wi = _ytables(n, nb)
        c, s = _trig(n, n, n)
        cs = np.concatenate([c, s]).astype(np.float32)
        ut = jnp.transpose(u, (0, 2, 1))
        anyspec = pl.BlockSpec(memory_space=pl.ANY)
        vmspec = pl.BlockSpec(memory_space=pltpu.VMEM)
        dma = pltpu.SemaphoreType.DMA
        vm = lambda *shape: pltpu.VMEM(shape, F32)
        acc, ql = pl.pallas_call(
            functools.partial(_spectral, nb), name="spectral",
            in_specs=[pl.BlockSpec(memory_space=pltpu.HBM)] * 8, out_specs=[vmspec] * 2,
            out_shape=[vm(nz, n, ZT, ya), vm(nz, klast, ZT, ya)],
            scratch_shapes=[
                vm(3, n, ZT, ya), vm(nz, na, ROWS, ZT, ya), vm(nz, ROWS, ZT, ya),
                vm(nkx, nb, zb, 128), vm(nkx, n, 128), vm(nkx, nb, zb, 128),
                vm(2, KC, *g.shape[1:]),
                vm(*tf.shape), vm(*wy.shape), vm(*cs.shape), vm(*bulk.shape),
                pltpu.VMEM((3, *tf.shape), BF16), pltpu.VMEM((3, *wy.shape), BF16), pltpu.VMEM((3, *wi.shape), BF16),
                pltpu.VMEM(last.shape, BF16),
                dma((6,)), dma((3,)), dma((2,)), dma((nz,)), dma((nz,)), dma((3, NA * npiece)), dma((3, NA * npiece)),
                dma((3, nchunk)), dma((3, nchunk)), dma((3, nchunk + SL)), dma((3, nchunk + SL)),
                dma((nchunk + SL,)), dma((nchunk + SL,)), dma((npiece,)), dma((npiece,)),
            ],
            compiler_params=pltpu.CompilerParams(
                collective_id=0, has_side_effects=True, vmem_limit_bytes=53 << 20),
        )(ut, g, tf, wy, cs, wi, bulk, last)
        w = pl.pallas_call(
            _finish, name="finish",
            in_specs=[vmspec] * 3, out_specs=anyspec,
            out_shape=jax.ShapeDtypeStruct((n, zb, ya), F32),
            scratch_shapes=[vm(nz // SL, n, ZT, ya), dma((nz,))],
            compiler_params=pltpu.CompilerParams(vmem_limit_bytes=24 << 20),
        )(last, acc, ql)
        return jnp.transpose(w, (0, 2, 1))

    return jax.shard_map(local, mesh=mesh, in_specs=(P(None, "a", "b"), P("a", "b", None)), out_specs=P(None, "a", "b"), check_vma=False)
```

```python
import functools
import math
import jax
import jax.numpy as jnp
import numpy as np
from jax import lax
from jax.experimental import pallas as pl
from jax.experimental.pallas import tpu as pltpu
from jax.sharding import PartitionSpec as P

HI = lax.Precision.HIGHEST
F32, BF16 = jnp.float32, jnp.bfloat16
MESH = pl.DeviceIdType.MESH
KC = 5
KA = 13
NLAST = 4
ZT = 8
ROWS = 136
TROWS = 144
NA = 2
NS = 3
SL = 8


def _trig(n, rows, cols):
    r = np.arange(rows)[:, None]
    c = np.arange(cols)[None, :]
    ang = ((r * c) % n).astype(np.float32) * np.float32(2.0 * math.pi / n)
    return np.cos(ang.astype(np.float64)), np.sin(ang.astype(np.float64))


def _xforward(n, kx, na):
    cx, sx = _trig(n, kx, n)
    keep = (np.arange(kx) <= n // 2).astype(np.float64)[:, None]
    t = np.stack([cx * keep, -sx * keep]).reshape(2, na, -1, KA, n).transpose(1, 2, 0, 3, 4).reshape(na, -1, n)
    t = np.pad(t, ((0, 0), (0, TROWS - t.shape[1]), (0, 0)))
    return np.concatenate([t, t[:1]]).reshape((na + 1) * TROWS, n).astype(np.float32)


def _xinverse(n, kx, na):
    cx, sx = _trig(n, kx, n)
    k = np.arange(kx)
    wgt = (np.where((k == 0) | (k == n // 2), 1.0, 2.0) * (k <= n // 2) / n)[:, None]
    t = np.stack([cx * wgt, -sx * wgt], 1).reshape(na, kx // na, 2 * n)
    ends = list(range(0, kx // na - NS * KC + 1, KC)) + [kx // na]
    t = np.concatenate([t[:, i:j].reshape(-1, n) for i, j in zip(ends, ends[1:])])
    return t.T.astype(np.float32).copy()


def _ytables(n, nb):
    c, s = _trig(n, n, n)
    full = np.block([[c, -s], [s, c]])
    w = full.reshape(2 * n, 2, nb, n // nb).transpose(0, 2, 1, 3).reshape(2 * n, 2 * n)
    inv = (full.T / n).reshape(2, nb, n // nb, 2 * n).transpose(1, 0, 2, 3)
    inv = inv.reshape(2 * n, 2, 2, n // 2).transpose(0, 2, 1, 3).reshape(2 * n, 2 * n)
    return w.astype(np.float32), inv.astype(np.float32)


def _split(x):
    hi = x.astype(BF16)
    x = x - hi.astype(F32)
    mid = x.astype(BF16)
    return hi, mid, (x - mid.astype(F32)).astype(BF16)


def _nsplit(x):
    hi = x.astype(jnp.bfloat16)
    x = x - hi.astype(np.float32)
    mid = x.astype(jnp.bfloat16)
    return hi, mid, (x - mid.astype(np.float32)).astype(jnp.bfloat16)


def _mm(p, q):
    d = functools.partial(jnp.dot, preferred_element_type=F32)
    return d(p[0], q[2]) + d(p[1], q[1]) + d(p[2], q[0]) + d(p[0], q[1]) + d(p[1], q[0]) + d(p[0], q[0])


def _dot(p, q):
    return jnp.dot(p, q, precision=HI, preferred_element_type=F32)


def _cat(parts):
    return jnp.concatenate(parts, axis=1)


def _add_last(t_ref, q_ref, qrow, k, acc_ref, row, dst_ref, drow, x):
    for z in range(0, ZT, 2):
        hi, mid, lo = _split(_cat([q_ref[pl.ds(qrow + z + j, k, stride=ZT), :] for j in range(2)]))
        rhs = jnp.concatenate([s.astype(F32) for s in (lo, mid, hi, mid, hi, hi)], axis=0).astype(BF16)
        out = jnp.dot(t_ref[...], rhs, preferred_element_type=F32)
        for j in range(2):
            part = acc_ref[pl.ds(row + z + j, x, stride=ZT), :] + out[:, j * 128:(j + 1) * 128]
            dst_ref[pl.ds(drow + z + j, x, stride=ZT), :] = part


def _spectral(nb, u_ref, g_ref, t_ref, wy_ref, cs_ref, wi_ref, ai_ref, al_ref, acc_ref, ql_ref,
              uv, xb, ps, sf, r, v, gv, tv, wv, csv, aiv, tsp, wysp, wisp, alv,
              load_sem, u_sem, g_sem, xa_send, xa_recv, fa_send, fa_recv, f_send, f_recv,
              b_send, b_recv, q_send, q_recv, xp_send, xp_recv):
    b, a = lax.axis_index("b"), lax.axis_index("a")
    other = 1 - a
    nkx = g_ref.shape[0]
    nchunk, npiece = nkx // KC, nkx // KA
    nbulk = nchunk - NLAST
    n = r.shape[1]
    zb = n // nb
    nz = zb // ZT
    y = 128
    za, zr = NA * ZT, zb - NA * ZT
    npad = 2 * nkx - n // 2 - 1
    bx, by = lax.rem(b, 2), lax.div(b, 2)
    peers = [lax.rem(by + d // 2, 2) * 2 + lax.rem(bx + d % 2, 2) for d in (3, 1, 2)]
    us = uv.shape[0]

    def ck(i):
        return pl.ds(i * KC, KC)

    def ka(i):
        return pl.ds(i * KA, KA)

    loads = [pltpu.make_async_copy(s, d, load_sem.at[i]) for i, (s, d) in enumerate(
        [(t_ref, tv), (wy_ref, wv), (wi_ref, wv), (cs_ref, csv), (ai_ref, aiv), (al_ref, alv)])]
    gs = gv.shape[0]

    def gload(i):
        return pltpu.make_async_copy(g_ref.at[ck(i)], gv.at[lax.rem(i, gs)], g_sem.at[lax.rem(i, gs)])

    def uload(z):
        return pltpu.make_async_copy(
            u_ref.at[:, pl.ds(z * ZT, ZT)], uv.at[lax.rem(z, us)], u_sem.at[lax.rem(z, us)])

    def xremote(z):
        return pltpu.make_async_remote_copy(
            ps.at[z], xb.at[z, a], xa_send.at[z], xa_recv.at[z], device_id=(b, other), device_id_type=MESH)

    def xpiece(i):
        rows = pl.ds(i * 2 * KA, 2 * KA)
        return pltpu.make_async_remote_copy(
            ps.at[0, rows], xb.at[0, a, rows], xp_send.at[i], xp_recv.at[i],
            device_id=(b, other), device_id_type=MESH)

    def fwda(e, i, d, k):
        rows = pl.ds(i * KA, k)
        return pltpu.make_async_remote_copy(
            sf.at[rows, peers[d], pl.ds(e * ZT, ZT)], r.at[rows, pl.ds(b * zb + e * ZT, ZT)],
            fa_send.at[d, e * npiece + i], fa_recv.at[d, e * npiece + i],
            device_id=(peers[d], a), device_id_type=MESH)

    def fwd(i, d, k):
        rows = pl.ds(i * KC, k)
        return pltpu.make_async_remote_copy(
            sf.at[rows, peers[d], pl.ds(za, zr)], r.at[rows, pl.ds(b * zb + za, zr)],
            f_send.at[d, i], f_recv.at[d, i], device_id=(peers[d], a), device_id_type=MESH)

    def bwd(i, d, k):
        rows = pl.ds(i * KC, k)
        return pltpu.make_async_remote_copy(
            r.at[rows, pl.ds(peers[d] * zb, zb)], v.at[rows, b], b_send.at[d, i], b_recv.at[d, i],
            device_id=(peers[d], a), device_id_type=MESH)

    zs, nzi = zb // SL, nz // SL
    nwhole, nk = nchunk - NS, NS * KC
    k0 = nkx - nk
    qlrow = (nwhole - nbulk) * 4 * KC + a * 2 * nk

    def bwdl(p, d, k):
        rows = pl.ds(k0, k)
        return pltpu.make_async_remote_copy(
            r.at[rows, pl.ds(peers[d] * zb + p * zs, zs)], v.at[rows, b, pl.ds(p * zs, zs)],
            b_send.at[d, nwhole + p], b_recv.at[d, nwhole + p],
            device_id=(peers[d], a), device_id_type=MESH)

    def sized(short, full, act):
        @pl.when(jnp.logical_not(short))
        def _():
            act(full)

        @pl.when(short)
        def _():
            act(full - npad)

    def each(i, full, last, act):
        sized(jnp.logical_and(i == last, a == 1), full, lambda k: [act(d, k) for d in range(3)])

    def eacha(i, act):
        each(i, KA, npiece - 1, act)

    def eachc(i, act):
        each(i, KC, nchunk - 1, act)

    def qsrc(i):
        return ps.at[:, pl.ds(i * 2 * KC, 2 * KC)]

    def qremote(i):
        return pltpu.make_async_remote_copy(
            qsrc(i), acc_ref.at[:, pl.ds((i * 2 + a) * 2 * KC, 2 * KC)], q_send.at[i], q_recv.at[i],
            device_id=(b, other), device_id_type=MESH)

    def qlast(i):
        rows = pl.ds(((i - nbulk) * 2 + a) * 2 * KC, 2 * KC)
        return pltpu.make_async_remote_copy(
            qsrc(i), ql_ref.at[:, rows], q_send.at[i], q_recv.at[i], device_id=(b, other), device_id_type=MESH)

    def qslice(p):
        zi = pl.ds(p * nzi, nzi)
        return pltpu.make_async_remote_copy(
            ps.at[zi, pl.ds(k0 * 2, nk * 2)], ql_ref.at[zi, pl.ds(qlrow, nk * 2)],
            q_send.at[nwhole + p], q_recv.at[nwhole + p], device_id=(b, other), device_id_type=MESH)

    barrier = pltpu.get_barrier_semaphore()
    for dev in [(b, other)] + [(pb, a) for pb in peers]:
        pl.semaphore_signal(barrier, inc=1, device_id=dev, device_id_type=MESH)
    uload(0).start()
    loads[0].start()
    loads[1].start()

    src = uv.reshape(us * n * ZT, y)
    own = xb.reshape(nz * 2 * ROWS * ZT, y)
    sent = ps.reshape(nz * ROWS * ZT, y)

    def split_table(dst, step):
        @pl.loop(0, wv.shape[0] // step)
        def _(i):
            rows = pl.ds(i * step, step)
            for m, part in enumerate(_split(wv[rows, :])):
                dst[m, rows, :] = part

    def xhalf(zi, z, rhs, first, dst, base):
        rows = pl.ds(pl.multiple_of(first * TROWS, 16), TROWS)
        out = _mm([tsp[m, rows, :] for m in range(3)], rhs)
        for i in range(2):
            dst[pl.ds(base * ROWS * ZT + z + i, ROWS, stride=ZT), :] = out[:ROWS, i * y:(i + 1) * y]

    def xblock(zi, halves):
        slot = lax.rem(zi, us)
        for z in range(0, ZT, 2):
            rhs = _split(_cat([src[pl.ds(slot * n * ZT + z + i, n, stride=ZT), :] for i in range(2)]))
            if 1 in halves:
                xhalf(zi, z, rhs, a + 1, sent, zi)
            if 0 in halves:
                xhalf(zi, z, rhs, a, own, zi * 2 + a)

    loads[0].wait()
    for m, part in enumerate(_split(tv[...])):
        tsp[m] = part
    uload(0).wait()
    for z in range(1, us):
        uload(z).start()
    for c in loads[3:]:
        c.start()
    for i in range(gs):
        gload(i).start()
    xblock(0, (1,))
    pl.semaphore_wait(barrier, 4)

    @pl.loop(0, npiece)
    def _(i):
        xpiece(i).start()

    xblock(0, (0,))
    loads[1].wait()
    split_table(wysp, 128)
    loads[2].start()

    @pl.loop(0, NA)
    def _(e):
        @pl.when(e > 0)
        def _():
            xremote(e).wait_recv()

        @pl.loop(0, npiece)
        def _(i):
            @pl.when(e == 0)
            def _():
                xpiece(i).wait_recv()
            x = _split(_cat([xb[e, h, pl.ds((2 * i + c) * KA, KA)].reshape(KA * ZT, y)
                             for c in range(2) for h in range(2)]))
            out = _mm(x, [wysp[m] for m in range(3)])
            zrow = pl.multiple_of(e * ZT, ZT)
            for k in range(nb):
                sf[ka(i), k, pl.ds(zrow, ZT)] = out[:, k * y:(k + 1) * y].reshape(KA, ZT, y)
            r[ka(i), pl.ds(b * zb + zrow, ZT)] = sf[ka(i), b, pl.ds(zrow, ZT)]
            eacha(i, lambda d, k: fwda(e, i, d, k).start())

        @pl.loop(1 + 2 * e, 3 + (nz - 3) * e)
        def _(z):
            @pl.when(z + us - 1 < nz)
            def _():
                uload(z + us - 1).start()
            uload(z).wait()
            xblock(z, (1, 0))
            xremote(z).start()

    @pl.loop(NA, nz)
    def _(z):
        xremote(z).wait_recv()

    def xrow(k, c):
        return (lax.div(k, KA) * 2 + c) * KA + lax.rem(k, KA)

    @pl.loop(0, nchunk)
    def _(i):
        x = _cat([jnp.concatenate([xb[pl.ds(NA, nz - NA), h, xrow(i * KC + j, c)].reshape(zr, y) for j in range(KC)])
                  for c in range(2) for h in range(2)])
        out = _mm(_split(x), [wysp[m] for m in range(3)])
        for k in range(nb):
            sf[ck(i), k, pl.ds(za, zr)] = out[:, k * y:(k + 1) * y].reshape(KC, zr, y)
        r[ck(i), pl.ds(b * zb + za, zr)] = sf[ck(i), b, pl.ds(za, zr)]
        eachc(i, lambda d, k: fwd(i, d, k).start())

    @pl.when(a == 1)
    def _():
        for k in range(npad):
            r[nkx - 1 - k] = jnp.zeros((n, y), F32)
            v[nkx - 1 - k] = jnp.zeros((nb, zb, y), F32)

    for c in loads[2:]:
        c.wait()
    split_table(wisp, 128)
    lane = lax.broadcasted_iota(jnp.int32, (n, y), 1)
    sign = jnp.where(lane < y // 2, 1.0, -1.0).astype(F32)

    @pl.loop(0, NA)
    def _(e):
        @pl.loop(0, npiece)
        def _(i):
            eacha(i, lambda d, k: fwda(e, i, d, k).wait_recv())

    @pl.loop(0, nchunk)
    def _(i):
        eachc(i, lambda d, k: fwd(i, d, k).wait_recv())
        gload(i).wait()
        e = _dot(csv[...], _cat([r[i * KC + j] for j in range(KC)]))
        parts = []
        for j in range(KC):
            cols = slice(j * y, (j + 1) * y)
            g1 = gv[lax.rem(i, gs), j] * (1.0 / n)
            gt = jnp.transpose(jnp.concatenate([g1, g1], axis=0))
            parts.append((e[:n, cols] + sign * pltpu.roll(e[n:, cols], y // 2, 1)) * gt)

        @pl.when(i + gs < nchunk)
        def _():
            gload(i + gs).start()
        e = _dot(csv[...], _cat(parts))
        for j in range(KC):
            cols = slice(j * y, (j + 1) * y)
            r[i * KC + j] = e[:n, cols] - sign * pltpu.roll(e[n:, cols], y // 2, 1)
        v[ck(i), b] = r[ck(i), pl.ds(b * zb, zb)]

        @pl.when(i < nwhole)
        def _():
            for d in range(3):
                bwd(i, d, KC).start()

    @pl.loop(0, SL)
    def _(p):
        sized(a == 1, nk, lambda k: [bwdl(p, d, k).start() for d in range(3)])

    @pl.loop(0, npiece)
    def _(i):
        xpiece(i).wait_send()

    @pl.loop(1, nz)
    def _(z):
        xremote(z).wait_send()

    def yinverse(k, nk, own_ref, row, p, zs):
        z0, nzi = pl.multiple_of(p * zs, ZT), zs // ZT
        zi = pl.ds(p * nzi, nzi)
        x = _cat([v[pl.ds(k, nk), m, pl.ds(z0, zs)].reshape(nk * zs, y) for m in range(nb)])
        out = _mm(_split(x), [wisp[m] for m in range(3)])

        def tile(h, c, j):
            m = h * 2 + c
            return out[j * zs:(j + 1) * zs, m * y:(m + 1) * y].reshape(nzi, ZT, y)

        for c in range(2):
            for j in range(nk):
                t0, t1 = tile(0, c, j), tile(1, c, j)
                own_ref[zi, row + j * 2 + c] = jnp.where(a == 0, t0, t1)
                ps[zi, k * 2 + j * 2 + c] = jnp.where(a == 0, t1, t0)

    @pl.loop(0, nbulk)
    def _(i):
        for d in range(3):
            bwd(i, d, KC).wait_recv()
        yinverse(i * KC, KC, acc_ref, (i * 2 + a) * 2 * KC, 0, zb)
        qremote(i).start()

    @pl.loop(0, nbulk)
    def _(i):
        qremote(i).wait_recv()

    brows = nbulk * 4 * KC
    arows = acc_ref.shape[1]
    flat = acc_ref.reshape(nz * arows * ZT, y)

    @pl.loop(0, nz)
    def _(zi):
        for z in range(0, ZT, 2):
            rhs = _cat([flat[pl.ds(zi * arows * ZT + z + i, brows, stride=ZT), :] for i in range(2)])
            out = _dot(aiv[...], rhs)
            for i in range(2):
                flat[pl.ds(zi * arows * ZT + z + i, arows, stride=ZT), :] = out[:, i * y:(i + 1) * y]

    @pl.loop(nbulk, nwhole)
    def _(i):
        for d in range(3):
            bwd(i, d, KC).wait_recv()
        yinverse(i * KC, KC, ql_ref, ((i - nbulk) * 2 + a) * 2 * KC, 0, zb)
        qlast(i).start()

    krows = ql_ref.shape[1]
    qflat = ql_ref.reshape(nz * krows * ZT, y)

    @pl.loop(nbulk, nwhole)
    def _(i):
        qlast(i).wait_recv()

    @pl.loop(0, SL)
    def _(p):
        sized(a == 1, nk, lambda k: [bwdl(p, d, k).wait_recv() for d in range(3)])
        yinverse(k0, nk, ql_ref, qlrow, p, zs)
        qslice(p).start()

        @pl.when(p > 0)
        def _():
            qslice(p - 1).wait_recv()

            @pl.loop((p - 1) * nzi, p * nzi)
            def _(zi):
                _add_last(alv, qflat, zi * krows * ZT, krows, flat, zi * arows * ZT, flat, zi * arows * ZT, arows)

    @pl.loop(0, NA)
    def _(e):
        @pl.loop(0, npiece)
        def _(i):
            eacha(i, lambda d, k: fwda(e, i, d, k).wait_send())

    @pl.loop(0, nchunk)
    def _(i):
        eachc(i, lambda d, k: fwd(i, d, k).wait_send())

    @pl.loop(0, nwhole)
    def _(i):
        for d in range(3):
            bwd(i, d, KC).wait_send()

    @pl.loop(0, nbulk)
    def _(i):
        qremote(i).wait_send()

    @pl.loop(nbulk, nwhole)
    def _(i):
        qlast(i).wait_send()

    @pl.loop(0, SL)
    def _(p):
        sized(a == 1, nk, lambda k: [bwdl(p, d, k).wait_send() for d in range(3)])
        qslice(p).wait_send()

    qslice(SL - 1).wait_recv()


def _finish(t_ref, w_ref, q_ref, o_ref, ov, out_sem):
    nz, x, zt, y = w_ref.shape
    k = q_ref.shape[1]
    rest = ov.shape[0]
    src = q_ref.reshape(nz * k * zt, y)
    acc = w_ref.reshape(nz * x * zt, y)
    dst = ov.reshape(rest * x * zt, y)

    def store(i, ref):
        return pltpu.make_async_copy(ref, o_ref.at[:, pl.ds(i * zt, zt)], out_sem.at[i])

    for i in range(nz - rest):
        store(i, w_ref.at[i]).start()
    for j in range(rest):
        i = nz - rest + j
        _add_last(t_ref, src, i * k * zt, k, acc, i * x * zt, dst, j * x * zt, x)
        store(i, ov.at[j]).start()
    for i in range(nz - rest):
        store(i, w_ref.at[i]).wait()
    for j in range(rest):
        store(nz - rest + j, ov.at[j]).wait()


def solution(mesh):
    na, nb = mesh.shape["a"], mesh.shape["b"]

    def local(u, g):
        n, ya, zb = u.shape
        nkx = g.shape[0]
        kx = nkx * na
        nchunk, npiece, nz = nkx // KC, nkx // KA, zb // ZT
        klast = NLAST * na * 2 * KC
        brows = (nchunk - NLAST) * 4 * KC
        tf, ti = _xforward(n, kx, na), _xinverse(n, kx, na)
        bulk = np.ascontiguousarray(ti[:, :brows])
        hi, mid, lo = _nsplit(ti[:, brows:])
        last = np.concatenate([hi, mid, lo, hi, mid, hi], axis=1)
        wy, wi = _ytables(n, nb)
        c, s = _trig(n, n, n)
        cs = np.concatenate([c, s]).astype(np.float32)
        ut = jnp.transpose(u, (0, 2, 1))
        anyspec = pl.BlockSpec(memory_space=pl.ANY)
        vmspec = pl.BlockSpec(memory_space=pltpu.VMEM)
        dma = pltpu.SemaphoreType.DMA
        vm = lambda *shape: pltpu.VMEM(shape, F32)
        acc, ql = pl.pallas_call(
            functools.partial(_spectral, nb), name="spectral",
            in_specs=[pl.BlockSpec(memory_space=pltpu.HBM)] * 8, out_specs=[vmspec] * 2,
            out_shape=[vm(nz, n, ZT, ya), vm(nz, klast, ZT, ya)],
            scratch_shapes=[
                vm(3, n, ZT, ya), vm(nz, na, ROWS, ZT, ya), vm(nz, ROWS, ZT, ya),
                vm(nkx, nb, zb, 128), vm(nkx, n, 128), vm(nkx, nb, zb, 128),
                vm(2, KC, *g.shape[1:]),
                vm(*tf.shape), vm(*wy.shape), vm(*cs.shape), vm(*bulk.shape),
                pltpu.VMEM((3, *tf.shape), BF16), pltpu.VMEM((3, *wy.shape), BF16), pltpu.VMEM((3, *wi.shape), BF16),
                pltpu.VMEM(last.shape, BF16),
                dma((6,)), dma((3,)), dma((2,)), dma((nz,)), dma((nz,)), dma((3, NA * npiece)), dma((3, NA * npiece)),
                dma((3, nchunk)), dma((3, nchunk)), dma((3, nchunk + SL)), dma((3, nchunk + SL)),
                dma((nchunk + SL,)), dma((nchunk + SL,)), dma((npiece,)), dma((npiece,)),
            ],
            compiler_params=pltpu.CompilerParams(
                collective_id=0, has_side_effects=True, vmem_limit_bytes=53 << 20),
        )(ut, g, tf, wy, cs, wi, bulk, last)
        w = pl.pallas_call(
            _finish, name="finish",
            in_specs=[vmspec] * 3, out_specs=anyspec,
            out_shape=jax.ShapeDtypeStruct((n, zb, ya), F32),
            scratch_shapes=[vm(nz // SL, n, ZT, ya), dma((nz,))],
            compiler_params=pltpu.CompilerParams(vmem_limit_bytes=24 << 20),
        )(last, acc, ql)
        return jnp.transpose(w, (0, 2, 1))

    return jax.shard_map(local, mesh=mesh, in_specs=(P(None, "a", "b"), P("a", "b", None)), out_specs=P(None, "a", "b"), check_vma=False)
```
